32 devices in a mesh: section: 4 (over y, x), seq: 2 (over core), dp: 4 (over z).
Axes of the slice: x: 2, y: 2, z: 4, core: 2. Of those that a mesh axis runs over, the one named last changes fastest.
Arguments:
- stream: bfloat16 [4, 4, 256, 1280], P('section', 'dp', 'seq'), may hold values from -16 to 16
- norm_gain: float32 [4, 1280], P('section'), may hold values from 0.25 to 1.75
- w_xbc: bfloat16 [4, 1280, 2688], P('section', ('seq', 'dp')), may hold values from -0.15625 to 0.15625
- w_dt: bfloat16 [4, 1280, 40], P('section', ('seq', 'dp')), may hold values from -0.15625 to 0.15625
- conv_weight: float32 [4, 4, 2688], P('section'), may hold values from -3 to 3
- conv_bias: float32 [4, 2688], P('section'), may hold values from -1.8 to 1.8
- dt_bias: float32 [4, 40], P('section'), may hold values from -1 to 1
- decay_rate: float32 [4, 40], P('section'), may hold values from 0.000390625 to 0.04
- skip_weight: float32 [4, 40], P('section'), may hold values from 0.5 to 1.5
- inner_gain: float32 [4, 2560], P('section'), may hold values from 0.25 to 1.75
- w_out: bfloat16 [4, 2560, 1280], P('section', ('seq', 'dp')), may hold values from -0.125 to 0.125
Outputs:
- next_stream: bfloat16 [4, 4, 256, 1280], P('section', 'dp', 'seq')
The draws below stay inside these ranges and needn't reach their ends.
All inputs are finite; a program needn't handle non-finite values.
Results may differ from the reference program's by a relative error of at most 0.008.
Values may be sent and summed in bfloat16 or wider, within the bound.
A program may use at most 64 MiB of HBM per device.

```python
import math
import jax
import jax.numpy as jnp
from jax import lax

D = 1280
HEADS = 40
HEAD_DIM = 64
STATE = 64
CONV = 4
BLOCK = 128
INNER = 2560
CH = 2688
LENGTH = 256
N_SECTION = 4
N_DP = 4


def draw_stream(key, part):
    base_key, row_key, col_key = jax.random.split(key, 3)
    full_shape = (N_SECTION, N_DP, LENGTH, D)
    row_scale = 10.0 ** jax.random.uniform(row_key, (N_SECTION, N_DP, LENGTH, 1), minval=-0.8, maxval=0.2)
    col_scale = 10.0 ** jax.random.uniform(col_key, (1, 1, 1, D), minval=-0.25, maxval=0.25)
    base_values = jax.random.normal(base_key, full_shape)
    return jnp.clip(base_values * row_scale * col_scale, -16.0, 16.0).astype(jnp.bfloat16)


def block_scale(stream_key, extent, cuts, low, high):
    level = 1.0
    for position, shards_of in cuts:
        steps = jax.random.uniform(jax.random.fold_in(jax.random.fold_in(stream_key, 6), position), (shards_of,), jnp.float32, low / len(cuts), high / len(cuts))
        level = level * jnp.repeat(jnp.exp(steps), extent[position] // shards_of).reshape((-1,) + (1,) * (len(extent) - 1 - position))
    return level


def centred(key, shape, deviation, reach, cuts=(), held_as=jnp.bfloat16):
    entries = jax.random.normal(key, shape, jnp.float32) * deviation
    if len(cuts) > 0:
        entries = block_scale(key, shape, cuts, -0.22, 0.18) * entries
    return jnp.clip(entries, min=-reach, max=reach).astype(held_as)


def setup_inputs(seed: int = 0) -> dict:
    key_list = jax.random.split(jax.random.key(seed), 12)
    return {
        "stream": draw_stream(jax.random.fold_in(key_list[11], 71), 0),
        "norm_gain": jnp.clip(1.0 + 0.15 * jax.random.normal(key_list[1], (N_SECTION, D), jnp.float32), 0.25, 1.75),
        "w_xbc": centred(key_list[2], (N_SECTION, D, CH), D ** -0.5, 0.15625, ((0, 4), (1, 8))),
        "w_dt": centred(key_list[3], (N_SECTION, D, HEADS), D ** -0.5, 0.15625, ((0, 4), (1, 8))),
        "conv_weight": centred(key_list[4], (N_SECTION, CONV, CH), CONV ** -0.5, 3.0, ((0, 4),), jnp.float32),
        "conv_bias": centred(key_list[5], (N_SECTION, CH), 0.3, 1.8, ((0, 4),), jnp.float32),
        "dt_bias": jnp.clip(jax.random.uniform(key_list[6], (N_SECTION, HEADS), jnp.float32, -1.0, 1.0) * block_scale(key_list[6], (N_SECTION, HEADS), ((0, 4),), -0.4, 0.0), -1.0, 1.0),
        "decay_rate": jnp.clip(jnp.exp(math.log(0.04) - 4.6288867 * jax.random.uniform(key_list[7], (N_SECTION, HEADS), jnp.float32) ** block_scale(key_list[7], (N_SECTION, HEADS), ((0, 4),), -0.2, 0.2)), 0.000390625, 0.04),
        "skip_weight": jnp.clip(0.5 + 1.0 * jax.random.uniform(key_list[8], (N_SECTION, HEADS), jnp.float32) ** block_scale(key_list[8], (N_SECTION, HEADS), ((0, 4),), -0.2, 0.2), 0.5, 1.5),
        "inner_gain": jnp.clip(1.0 + 0.15 * jax.random.normal(key_list[9], (N_SECTION, INNER), jnp.float32), 0.25, 1.75),
        "w_out": centred(key_list[10], (N_SECTION, INNER, D), INNER ** -0.5, 0.125, ((0, 4), (1, 8))),
    }


epsilon = 1e-05

def rms_scale(values, scale_gain):
    mean_square = lax.optimization_barrier(jnp.mean(values * values, axis=-1, keepdims=True))
    return values * lax.rsqrt(mean_square + epsilon) * scale_gain

def block_terms(values, b_rows, c_rows, dt_rows, head_rates):
    block_len = dt_rows.shape[0]
    cum_decay = jnp.cumsum(-dt_rows * head_rates[None, :], axis=0)
    scores = jnp.dot(c_rows, b_rows.T, preferred_element_type=jnp.float32)
    lag_decay = cum_decay.T[:, :, None] - cum_decay.T[:, None, :]
    causal = jnp.arange(block_len)[:, None] >= jnp.arange(block_len)[None, :]
    weights = jnp.where(causal[None], jnp.exp(jnp.minimum(lag_decay, 0.0)), 0.0)
    mixing = (scores[None] * weights * dt_rows.T[:, None, :]).astype(jnp.bfloat16)
    intra_out = jnp.einsum('hij,jhp->ihp', mixing.astype(jnp.float32), values.astype(jnp.float32))
    tail_weight = jnp.exp(cum_decay[-1][None, :] - cum_decay) * dt_rows
    scaled = (values.astype(jnp.float32) * tail_weight[:, :, None]).astype(jnp.bfloat16)
    summary = jnp.einsum('jhp,jn->hpn', scaled.astype(jnp.float32), b_rows.astype(jnp.float32))
    return (intra_out, summary, jnp.exp(cum_decay[-1]), jnp.exp(cum_decay))

def state_output(c_rows, growth, carried):
    readout = jnp.einsum('in,hpn->ihp', c_rows.astype(jnp.float32), carried, precision=lax.Precision.HIGHEST)
    return growth[:, :, None] * readout

def mamba_layer(seq_rows, row_gain, xbc_weight, dt_weight, tap_weight, tap_bias, dt_shift, head_rates, skip_gain, out_gain, out_weight):
    length_all = seq_rows.shape[0]
    blocks = length_all // BLOCK
    normed = rms_scale(seq_rows.astype(jnp.float32), row_gain).astype(jnp.bfloat16)
    xbc_raw = jnp.dot(normed, xbc_weight, preferred_element_type=jnp.float32).astype(jnp.bfloat16)
    dt_raw = jnp.dot(normed, dt_weight, preferred_element_type=jnp.float32)
    padded = jnp.concatenate([jnp.zeros((CONV - 1, xbc_raw.shape[1]), jnp.bfloat16), xbc_raw], axis=0)
    conv_sum = jnp.broadcast_to(tap_bias[None, :], xbc_raw.shape)
    for tap_index in range(CONV):
        conv_sum = conv_sum + tap_weight[tap_index][None, :] * padded[tap_index:tap_index + length_all].astype(jnp.float32)
    mixed_rows = jax.nn.silu(conv_sum).astype(jnp.bfloat16)
    values = mixed_rows[:, :INNER].reshape(blocks, BLOCK, HEADS, HEAD_DIM)
    b_rows = mixed_rows[:, INNER:INNER + STATE].reshape(blocks, BLOCK, STATE)
    c_rows = mixed_rows[:, INNER + STATE:].reshape(blocks, BLOCK, STATE)
    dt_rows = jax.nn.softplus(dt_raw + dt_shift[None, :]).reshape(blocks, BLOCK, HEADS)

    def block_step(carried, inputs):
        block_values, block_b, block_c, block_dt = inputs
        intra_out, summary, block_total, growth = block_terms(block_values, block_b, block_c, block_dt, head_rates)
        state_part = state_output(block_c, growth, carried)
        output = intra_out + state_part + skip_gain[None, :, None] * block_values.astype(jnp.float32)
        return (block_total[:, None, None] * carried + summary, output)
    zero_state = jnp.zeros((HEADS, HEAD_DIM, STATE), jnp.float32)
    final_state, outputs = lax.scan(block_step, zero_state, (values, b_rows, c_rows, dt_rows))
    normed_out = rms_scale(outputs.reshape(length_all, INNER), out_gain).astype(jnp.bfloat16)
    branch_out = jnp.dot(normed_out, out_weight, preferred_element_type=jnp.float32)
    return (seq_rows.astype(jnp.float32) + branch_out).astype(jnp.bfloat16)

def reference(stream, norm_gain, w_xbc, w_dt, conv_weight, conv_bias, dt_bias, decay_rate, skip_weight, inner_gain, w_out):

    def one_section(section_inputs):
        rows_all, row_gain, xbc_weight, dt_weight, tap_weight, tap_bias, dt_shift, head_rates, skip_gain, out_gain, out_weight = section_inputs

        def one_sequence(seq_rows):
            return mamba_layer(seq_rows, row_gain, xbc_weight, dt_weight, tap_weight, tap_bias, dt_shift, head_rates, skip_gain, out_gain, out_weight)
        return lax.map(one_sequence, rows_all)
    results = lax.map(one_section, (stream, norm_gain, w_xbc, w_dt, conv_weight, conv_bias, dt_bias, decay_rate, skip_weight, inner_gain, w_out))
    return jnp.roll(results, 1, axis=0)
```

```python
import functools

import jax
import jax.numpy as jnp
from jax import lax
from jax.experimental import pallas as pl
from jax.experimental.pallas import tpu as pltpu
from jax.sharding import PartitionSpec as P

HEADS = 40
HEAD_DIM = 64
STATE = 64
CONV = 4
BLOCK = 128
INNER = 2560


epsilon = 1e-05


def prefix(x, axis, combine, identity):
    devices, position = (lax.axis_size(axis), lax.axis_index(axis))
    everything = jax.tree.map(
        lambda part, kind: lax.all_gather(part.astype(kind), axis),
        x,
        jax.tree.map(lambda a: jnp.bfloat16 if a.dtype == jnp.float32 else a.dtype, x),
    )
    start = jax.tree.map(
        lambda part, zero: jnp.broadcast_to(jnp.asarray(zero, part.dtype), part.shape), x, identity
    )

    def hop(k, before):
        reached = k < position
        new = combine(
            before, jax.tree.map(lambda part, own: part[k].astype(own.dtype), everything, x)
        )
        return jax.tree.map(lambda a, b: jnp.where(reached, a, b), new, before)

    return lax.fori_loop(0, devices, hop, start)


def from_behind(x, axis, by):
    devices = lax.axis_size(axis)
    pairs = [(i, i + by) for i in range(devices) if 0 <= i + by < devices]
    return lax.ppermute(x, axis, pairs)


def passed_along(x, axis, by):
    devices = lax.axis_size(axis)
    return lax.ppermute(x, axis, [(i, (i + by) % devices) for i in range(devices)])


def rms_scale(values, scale_gain):
    mean_square = jnp.mean(values * values, axis=-1, keepdims=True)
    return values * lax.rsqrt(mean_square + epsilon) * scale_gain


def block_terms(values, b_rows, c_rows, dt_rows, head_rates):
    block_len = dt_rows.shape[0]
    cum_decay = jnp.cumsum(-dt_rows * head_rates[None, :], axis=0)
    scores = jnp.dot(c_rows, b_rows.T, preferred_element_type=jnp.float32)
    lag_decay = cum_decay.T[:, :, None] - cum_decay.T[:, None, :]
    causal = jnp.arange(block_len)[:, None] >= jnp.arange(block_len)[None, :]
    weights = jnp.where(causal[None], jnp.exp(jnp.minimum(lag_decay, 0.0)), 0.0)
    mixing = (scores[None] * weights * dt_rows.T[:, None, :]).astype(jnp.bfloat16)
    intra_out = jnp.einsum("hij,jhp->ihp", mixing, values, preferred_element_type=jnp.float32)
    tail_weight = jnp.exp(cum_decay[-1][None, :] - cum_decay) * dt_rows
    scaled = (values.astype(jnp.float32) * tail_weight[:, :, None]).astype(jnp.bfloat16)
    summary = jnp.einsum("jhp,jn->hpn", scaled, b_rows, preferred_element_type=jnp.float32)
    return (intra_out, summary, jnp.exp(cum_decay[-1]), jnp.exp(cum_decay))


def state_output(c_rows, growth, carried):
    readout = jnp.einsum(
        "in,hpn->ihp", c_rows.astype(jnp.float32), carried, precision=lax.Precision.HIGHEST
    )
    return growth[:, :, None] * readout


def combine_states(earlier, latest):
    decay_a, state_a = earlier
    decay_b, state_b = latest
    return (decay_a * decay_b, decay_b[:, None] * state_a + state_b)


def chain_states(summary):
    identity = (jnp.ones_like(summary[0]), jnp.zeros_like(summary[1]))
    return prefix(summary, "seq", combine_states, identity)


def project_rows(normed_rows, xbc_part, dt_part):
    return (
        jnp.dot(
            normed_rows,
            lax.all_gather(xbc_part, ("seq", "dp"), axis=0, tiled=True),
            preferred_element_type=jnp.float32,
        ),
        jnp.dot(
            normed_rows,
            lax.all_gather(dt_part, ("seq", "dp"), axis=0, tiled=True),
            preferred_element_type=jnp.float32,
        ),
    )


def shards(
    stream,
    norm_gain,
    w_xbc,
    w_dt,
    conv_weight,
    conv_bias,
    dt_bias,
    decay_rate,
    skip_weight,
    inner_gain,
    w_out,
):
    rows_in = stream[0, 0]
    length_dev = rows_in.shape[0]
    margin = CONV - 1
    row_gain = norm_gain[0]
    normed = rms_scale(rows_in.astype(jnp.float32), row_gain).astype(jnp.bfloat16)
    projected, dt_raw = project_rows(normed, w_xbc[0], w_dt[0])
    xbc_raw = projected.astype(jnp.bfloat16)
    prev_proj = from_behind(xbc_raw[length_dev - margin :], "seq", 1)
    padded = jnp.concatenate([prev_proj, xbc_raw], axis=0)
    conv_sum = jnp.broadcast_to(conv_bias[0][None, :], (length_dev, padded.shape[1]))
    for tap_index in range(CONV):
        conv_sum = conv_sum + conv_weight[0, tap_index][None, :] * padded[
            tap_index : tap_index + length_dev
        ].astype(jnp.float32)
    mixed_rows = jax.nn.silu(conv_sum).astype(jnp.bfloat16)
    blocks = length_dev // BLOCK
    values = mixed_rows[:, :INNER].reshape(blocks, BLOCK, HEADS, HEAD_DIM)
    b_rows = mixed_rows[:, INNER : INNER + STATE].reshape(blocks, BLOCK, STATE)
    c_rows = mixed_rows[:, INNER + STATE :].reshape(blocks, BLOCK, STATE)
    dt_rows = jax.nn.softplus(dt_raw + dt_bias[0][None, :]).reshape(blocks, BLOCK, HEADS)
    intra_out, summary, totals, growth = jax.vmap(block_terms, in_axes=(0, 0, 0, 0, None))(
        values, b_rows, c_rows, dt_rows, decay_rate[0]
    )

    def local_step(running, inputs):
        carried, decay_before = running
        block_total, block_summary = inputs
        return (
            (block_total[:, None, None] * carried + block_summary, decay_before * block_total),
            (carried, decay_before),
        )

    start_state = (
        jnp.zeros((HEADS, HEAD_DIM, STATE), jnp.float32),
        jnp.ones((HEADS,), jnp.float32),
    )
    (local_state, local_decay), (enter_local, decay_before) = lax.scan(
        local_step, start_state, (totals, summary)
    )
    state_terms = jax.vmap(state_output)
    early_terms = state_terms(c_rows, growth, enter_local)
    incoming_decay, incoming_flat = chain_states(
        (local_decay, local_state.reshape(HEADS, HEAD_DIM * STATE))
    )
    arriving = incoming_flat.reshape(HEADS, HEAD_DIM, STATE)
    late_terms = state_terms(c_rows, growth, decay_before[:, :, None, None] * arriving[None])
    state_part = early_terms + late_terms
    mixed_out = (
        intra_out + state_part + skip_weight[0][None, None, :, None] * values.astype(jnp.float32)
    )
    normed_out = rms_scale(mixed_out.reshape(length_dev, INNER), inner_gain[0]).astype(jnp.bfloat16)
    branch_out = jnp.dot(
        normed_out,
        lax.all_gather(w_out[0], ("seq", "dp"), axis=0, tiled=True),
        preferred_element_type=jnp.float32,
    )
    next_rows = (rows_in.astype(jnp.float32) + branch_out).astype(jnp.bfloat16)
    shifted = passed_along(next_rows, "section", 1)
    return shifted[None, None]

def section_kernel(
    Z, x_hbm, ng_hbm, w_hbm, wd_hbm, cw_hbm, cb_hbm, db_hbm, dr_hbm, sk_hbm, ig_hbm, wo_hbm,
    out_ref,
    x_ref, ng_ref, w_ref, wd_ref, cw_ref, cb_ref, db_ref, dr_ref, sk_ref, ig_ref, wo_ref, w2, wbuf, d2, dbuf, wobuf, sbuf, nbuf, cbuf, vbuf, ybuf, state,
    pbuf, stbuf, xpart, xstat, bpart, bstat, rpart, rstat, obuf,
    l_sem, w_send, w_recv, d_send, d_recv, f_send, f_recv, g_send, g_recv, o_send, o_recv,
    s_send, s_recv, h_send, p_send, p_recv, t_send, t_recv, x_recv, y_recv, b_send, c_send, q_send, b_recv,
    e_send, e_recv,
):
    z = lax.axis_index("dp")
    c = lax.axis_index("seq")
    sec = lax.axis_index("section")
    NS = lax.axis_size("section")
    nxt = lax.rem(sec + 1, NS)
    prv = lax.rem(sec + NS - 1, NS)
    S = Z // 2
    rows, D = x_ref.shape
    KR = w_ref.shape[0]
    per = INNER // (2 * Z)
    hper = HEADS // (2 * Z)
    VC = 2 * per
    NB = 2 * STATE
    CC = VC + NB
    f32, bf16 = jnp.float32, jnp.bfloat16
    own_core = lax.rem(z, 2) == c
    myslot = z // 2
    sib = {"seq": 1 - c}
    upper = z >= S
    border = jnp.where(upper, S, S - 1)

    def rcopy(src, dst, ss, rs, where):
        return pltpu.make_async_remote_copy(
            src_ref=src, dst_ref=dst, send_sem=ss, recv_sem=rs, device_id=where,
            device_id_type=pl.DeviceIdType.MESH,
        )

    loads = [
        pltpu.make_async_copy(src, dst, l_sem.at[i])
        for i, (src, dst) in enumerate((
            (x_hbm, x_ref), (w_hbm, w_ref), (wd_hbm, wd_ref), (wo_hbm, wo_ref), (ng_hbm, ng_ref),
            (cw_hbm, cw_ref), (cb_hbm, cb_ref), (db_hbm, db_ref), (dr_hbm, dr_ref), (sk_hbm, sk_ref),
            (ig_hbm, ig_ref)))
    ]
    for load in loads:
        load.start()
    barrier = pltpu.get_barrier_semaphore()
    for d in range(Z):
        for e in range(2):
            @pl.when(jnp.logical_not(jnp.logical_and(d == z, e == c)))
            def _():
                pl.semaphore_signal(barrier, inc=1, device_id={"dp": d, "seq": e},
                                    device_id_type=pl.DeviceIdType.MESH)
    for s in (nxt, prv):
        pl.semaphore_signal(barrier, inc=1, device_id={"section": s},
                            device_id_type=pl.DeviceIdType.MESH)

    def row0(core, chip):
        return pl.multiple_of((core * Z + chip) * KR, KR)

    lanes = d2.shape[2]
    loads[2].wait()
    for d in range(Z):
        two = jnp.concatenate(
            [wd_ref[d * hper : (d + 1) * hper, :].astype(f32),
             wd_ref[(Z + d) * hper : (Z + d + 1) * hper, :].astype(f32),
             jnp.zeros((16 - 2 * hper, KR), f32)], axis=0)
        d2[d] = jnp.concatenate([two, jnp.zeros((16, lanes - KR), f32)], axis=1).astype(bf16)
    dbuf[c * Z + z] = d2[z]
    loads[0].wait()

    @pl.when(own_core)
    def _():
        sbuf[myslot, c] = x_ref[...]

    loads[1].wait()
    for d in range(Z):
        w2[d, :, 0:per] = w_ref[:, d * per : (d + 1) * per]
        w2[d, :, per:VC] = w_ref[:, Z * per + d * per : Z * per + (d + 1) * per]
        w2[d, :, VC:CC] = w_ref[:, INNER : INNER + NB]

    pl.semaphore_wait(barrier, 2 * Z - 1 + 2)

    def s_copy(src, k, h, direction):
        return rcopy(src, sbuf.at[k, h], s_send.at[k, h, direction], s_recv.at[k, h],
                     {"dp": z + (1 if direction else -1)})

    half_out = rcopy(x_ref, sbuf.at[myslot, c], h_send, s_recv.at[myslot, c], sib)

    @pl.when(jnp.logical_not(own_core))
    def _():
        half_out.start()

    def up_down(k, h, fn):
        b = 2 * k + c
        @pl.when(jnp.logical_and(z >= b, z + 1 < Z))
        def _():
            fn(s_copy(sbuf.at[k, h], k, h, 1))
        @pl.when(jnp.logical_and(z <= b, z > 0))
        def _():
            fn(s_copy(sbuf.at[k, h], k, h, 0))

    def own_halves(across):
        for h in (c, 1 - c):
            if not across:
                @pl.when(jnp.logical_and(own_core, h != c))
                def _():
                    s_copy(x_ref, myslot, h, 0).wait_recv()
            for direction, on, edge in ((1, z + 1 < Z, S - 1), (0, z > 0, S)):
                cross = z == edge
                go = cross if across else jnp.logical_not(cross)
                @pl.when(jnp.logical_and(jnp.logical_and(own_core, on), go))
                def _():
                    s_copy(sbuf.at[myslot, h], myslot, h, direction).start()

    own_halves(False)

    def w_copies(d, frm):
        at = pl.ds(row0(c, frm), KR)
        g = c * Z + frm
        return (rcopy(w2.at[d], wbuf.at[at], w_send.at[d], w_recv.at[frm], {"dp": d}),
                rcopy(d2.at[d], dbuf.at[g], d_send.at[d], d_recv.at[frm], {"dp": d}))

    def f_copies(d, core):
        at = pl.ds(row0(core, d), KR)
        g = core * Z + d
        return (rcopy(wbuf.at[at], wbuf.at[at], f_send.at[d], f_recv.at[d], sib),
                rcopy(dbuf.at[g], dbuf.at[g], g_send.at[d], g_recv.at[d], sib))

    for step in range(Z - 1, 0, -1):
        for d in (z + step, z - step):
            @pl.when(jnp.logical_and(d >= 0, d < Z))
            def _():
                for cp in w_copies(d, z):
                    cp.start()
    own_halves(True)
    own_fwd = (
        rcopy(w2.at[z], wbuf.at[pl.ds(row0(c, z), KR)], f_send.at[z], f_recv.at[z], sib),
        rcopy(d2.at[z], dbuf.at[c * Z + z], g_send.at[z], g_recv.at[z], sib),
    )
    for cp in own_fwd:
        cp.start()
    wbuf[pl.ds(row0(c, z), KR), :] = w2[z]
    loads[3].wait()
    at_wo = pl.ds(pl.multiple_of(c * per, per), per)
    wo_copy = rcopy(wo_ref, wobuf.at[at_wo], o_send, o_recv, sib)
    wo_copy.start()
    wobuf[at_wo, :] = wo_ref[...]

    near = jnp.where(upper, S - 1, 0)
    for load in loads[4:]:
        load.wait()
    gain_in = ng_ref[...]

    def pass_on(k, h):
        @pl.when(jnp.logical_not(jnp.logical_and(own_core, k == myslot)))
        def _():
            s_copy(x_ref, k, h, 0).wait_recv()
            up_down(k, h, lambda cp: cp.start())

    def norm_in(k, h):
        v = sbuf[k, h].astype(f32)
        ms = jnp.mean(v * v, axis=-1, keepdims=True)
        nbuf[k, h] = (v * lax.rsqrt(ms + epsilon) * gain_in).astype(bf16)

    far = 1 - near
    for h in range(2):
        pass_on(near, h)
        norm_in(near, h)
    for step in range(1, Z):
        for d in (z + step, z - step):
            @pl.when(jnp.logical_and(d >= 0, d < Z))
            def _():
                for cp in w_copies(z, d):
                    cp.wait_recv()
                for cp in f_copies(d, c):
                    cp.start()

    def pick(ref, width, tail):
        wide = Z * width
        got = None
        for d in range(Z):
            part = jnp.concatenate(
                [ref[:, d * width : (d + 1) * width],
                 ref[:, wide + d * width : wide + (d + 1) * width]], axis=1)
            part = jnp.where(z == d, part, 0.0)
            got = part if got is None else got + part
        return jnp.concatenate([got, tail], axis=1) if tail is not None else got

    hi = lax.Precision.HIGHEST
    taps = pick(cw_ref, per, cw_ref[:, INNER : INNER + NB])
    tbias = pick(cb_ref, per, cb_ref[:, INNER : INNER + NB])
    hz = jnp.zeros((1, 128 - 2 * hper), f32)
    heads = jnp.concatenate(
        [pick(db_ref, hper, hz), pick(dr_ref, hper, hz), pick(sk_ref, hper, hz),
         jnp.zeros((5, 128), f32)], axis=0)
    heads_t = heads.T[0:16]
    dtb, rate = heads_t[:, 0:1], heads_t[:, 1:2]
    gain_out = pick(ig_ref, per, None)
    spread = (lax.broadcasted_iota(jnp.int32, (16, VC), 1) // HEAD_DIM
              == lax.broadcasted_iota(jnp.int32, (16, VC), 0)).astype(f32)

    def widen(m):
        return jnp.dot(m, spread, precision=hi, preferred_element_type=f32)

    skip_wide = widen(heads[:, 0:16])[2:3]
    ii = lax.broadcasted_iota(jnp.int32, (BLOCK, BLOCK), 0)
    jj = lax.broadcasted_iota(jnp.int32, (BLOCK, BLOCK), 1)
    causal = ii >= jj
    triu = (ii <= jj).astype(f32)
    low_lane = lax.broadcasted_iota(jnp.int32, (BLOCK, 128), 1) < HEAD_DIM
    margin = CONV - 1
    for d in range(Z):
        for cp in f_copies(d, 1 - c):
            cp.wait_recv()
    wo_copy.wait_recv()
    w_steps = jnp.concatenate([dbuf[g][:, 0:KR].astype(f32) for g in range(2 * Z)], axis=1).astype(bf16)

    def p_copies(k, h):
        b = 2 * k + c
        slot = lax.rem(z, S)
        return (rcopy(pbuf.at[k, h], rpart.at[slot], p_send.at[k, h], p_recv.at[slot], {"dp": b, "seq": h}),
                rcopy(stbuf.at[k, h], rstat.at[slot], t_send.at[k, h], t_recv.at[slot], {"dp": b, "seq": h}))

    half = rows // 2

    def x_copies(h, frm, q):
        slot = lax.rem(frm, S)
        at = pl.ds(q * half, half)
        big = rcopy(pbuf.at[far, h, at], xpart.at[slot, h, at], q_send.at[h, q], x_recv.at[slot, h, q], {"dp": border})
        if q > 0:
            return (big,)
        return (rcopy(stbuf.at[far, h], xstat.at[slot, h], t_send.at[far, h], y_recv.at[slot, h], {"dp": border}), big)

    def b_copies(h, q):
        where = {"dp": 2 * far + c, "seq": h}
        at = pl.ds(q * half, half)
        big = rcopy(bpart.at[h, at], rpart.at[S, at], b_send.at[h, q], b_recv.at[q], where)
        if q > 0:
            return (big,)
        return (rcopy(bstat.at[h], rstat.at[S], c_send.at[h], t_recv.at[S], where), big)

    def unit(k, h):
        nb = nbuf[k, h]
        if h == 0:
            cbuf[0:8, :] = jnp.zeros((8, CC), f32)
        else:
            cbuf[0:8, :] = cbuf[rows : rows + 8, :]
        cbuf[8 : 8 + rows, :] = jnp.dot(nb, wbuf[...], preferred_element_type=f32).astype(bf16).astype(f32)
        acc = jnp.broadcast_to(tbias, (rows, CC))
        for t in range(CONV):
            acc = acc + taps[t : t + 1, :] * cbuf[8 - margin + t : 8 - margin + t + rows, :]
        vbuf[...] = (acc / (1.0 + jnp.exp(-acc))).astype(bf16)
        raw = lax.dot_general(w_steps, nb, (((1,), (1,)), ((), ())), preferred_element_type=f32) + dtb
        dt_t = jnp.maximum(raw, 0.0) + jnp.log1p(jnp.exp(-jnp.abs(raw)))
        cum_t = jnp.dot(-dt_t * rate, triu, precision=hi, preferred_element_type=f32)
        tail_t = jnp.exp(cum_t[:, BLOCK - 1 : BLOCK] - cum_t) * dt_t
        cols = jnp.concatenate([cum_t, tail_t, jnp.exp(cum_t), jnp.zeros((80, BLOCK), f32)], axis=0).T
        cum = cols[:, 0:16]
        bm = vbuf[:, VC : VC + STATE]
        cm = vbuf[:, VC + STATE : CC]
        scores = lax.dot_general(cm, bm, (((1,), (1,)), ((), ())), preferred_element_type=f32)
        scores = jnp.where(causal, scores, 0.0)
        vals = vbuf[:, 0:VC].astype(f32)
        part = skip_wide * vals
        if h > 0:
            grow = widen(cols[:, 32:48])
            part = part + grow * jnp.dot(cm.astype(f32), state[...], precision=hi,
                                         preferred_element_type=f32)
        for p in range(VC // 128):
            mix = []
            for q in range(2):
                hd = 2 * p + q
                lag = cum[:, hd : hd + 1] - cum_t[hd : hd + 1, :]
                m = scores * jnp.exp(jnp.minimum(lag, 0.0)) * dt_t[hd : hd + 1, :]
                mix.append(m.astype(bf16))
            vp = vals[:, p * 128 : (p + 1) * 128]
            two = jnp.concatenate([jnp.where(low_lane, vp, 0.0), jnp.where(low_lane, 0.0, vp)],
                                  axis=0).astype(bf16)
            got = jnp.dot(jnp.concatenate(mix, axis=1), two, preferred_element_type=f32)
            ybuf[:, p * 128 : (p + 1) * 128] = got + part[:, p * 128 : (p + 1) * 128]
        y = ybuf[...]
        pbuf[k, h] = jnp.dot((y * gain_out).astype(bf16), wobuf[...], preferred_element_type=f32).astype(bf16)
        stbuf[k, h] = lax.dot_general(jnp.ones((8, VC), f32), y * y, (((1,), (1,)), ((), ())),
                                      precision=hi, preferred_element_type=f32)
        if h == 0:
            scaled = (vals * widen(cols[:, 16:32])).astype(bf16)
            state[...] = lax.dot_general(bm, scaled, (((0,), (0,)), ((), ())), preferred_element_type=f32)

    def send_far(h):
        @pl.when(z != border)
        def _():
            for q in range(2):
                for cp in x_copies(h, z, q):
                    cp.start()

    def sum_far(h):
        @pl.when(z == border)
        def _():
            for q in range(2):
                r = slice(q * half, (q + 1) * half)
                total = pbuf[far, h, r].astype(f32)
                stat = stbuf[far, h]
                for j in range(S):
                    frm = jnp.where(upper, S + j, j)
                    @pl.when(frm != border)
                    def _():
                        for cp in x_copies(h, frm, q):
                            cp.wait_recv()
                    total = total + jnp.where(frm == border, 0.0, xpart[j, h, r].astype(f32))
                    stat = stat + jnp.where(frm == border, 0.0, xstat[j, h])
                bpart[h, r] = total.astype(bf16)
                if q == 0:
                    bstat[h] = stat
                for cp in b_copies(h, q):
                    cp.start()

    def here(k, h):
        return jnp.logical_and(2 * k + c == z, h == c)

    def send_near(h, now):
        @pl.when(jnp.logical_and(now, here(near, h)))
        def _():
            rpart[lax.rem(z, S)] = pbuf[near, h]
            rstat[lax.rem(z, S)] = stbuf[near, h]

        @pl.when(jnp.logical_and(now, jnp.logical_not(here(near, h))))
        def _():
            for cp in p_copies(near, h):
                cp.start()

    for h in range(2):
        unit(near, h)
        send_near(h, z != border)
    for h in range(2):
        pass_on(far, h)
        norm_in(far, h)
        unit(far, h)
        send_far(h)
    for h in range(2):
        send_near(h, z == border)
    for h in range(2):
        sum_far(h)

    total = jnp.zeros((rows, D), f32)
    stat = jnp.zeros((8, rows), f32)
    for j in range(S + 1):
        mine = jnp.logical_and(own_core, lax.rem(z, S) == j) if j < S else False
        @pl.when(jnp.logical_not(mine))
        def _():
            if j == S:
                for q in range(2):
                    at = pl.ds(q * half, half)
                    rcopy(pbuf.at[0, 0, at], rpart.at[S, at], b_send.at[0, q], b_recv.at[q], sib).wait_recv()
            else:
                rcopy(pbuf.at[0, 0], rpart.at[j], p_send.at[0, 0], p_recv.at[j], sib).wait_recv()
            rcopy(stbuf.at[0, 0], rstat.at[j], t_send.at[0, 0], t_recv.at[j], sib).wait_recv()
        total = total + rpart[j].astype(f32)
        stat = stat + rstat[j]
    scale = lax.rsqrt(stat * (1.0 / INNER) + epsilon).T[:, 0:1]
    obuf[...] = (x_ref[...].astype(f32) + total * scale).astype(bf16)
    last_copy = rcopy(obuf, out_ref, e_send, e_recv, {"section": nxt})
    last_copy.start()

    @pl.when(jnp.logical_not(own_core))
    def _():
        half_out.wait_send()
    for cp in (*own_fwd, wo_copy):
        cp.wait_send()
    for d in range(Z):
        @pl.when(d != z)
        def _():
            for cp in (*w_copies(d, z), *f_copies(d, c)):
                cp.wait_send()
    for h in range(2):
        for k in range(S):
            up_down(k, h, lambda cp: cp.wait_send())
        @pl.when(z != border)
        def _():
            for cp in (*x_copies(h, z, 0), *x_copies(h, z, 1)):
                cp.wait_send()
        @pl.when(z == border)
        def _():
            for cp in (*b_copies(h, 0), *b_copies(h, 1)):
                cp.wait_send()
        @pl.when(jnp.logical_not(here(near, h)))
        def _():
            for cp in p_copies(near, h):
                cp.wait_send()
    last_copy.wait()


def fused(
    stream, norm_gain, w_xbc, w_dt, conv_weight, conv_bias, dt_bias, decay_rate, skip_weight,
    inner_gain, w_out,
):
    Z = lax.axis_size("dp")
    rows, D = stream.shape[2:]
    if rows != BLOCK:
        return shards(stream, norm_gain, w_xbc, w_dt, conv_weight, conv_bias, dt_bias, decay_rate,
                      skip_weight, inner_gain, w_out)
    KR = w_xbc.shape[1]
    VC = INNER // Z
    CC = VC + 2 * STATE
    S = Z // 2
    lanes = -(-KR // 128) * 128
    bf16, f32 = jnp.bfloat16, jnp.float32
    dma, V = pltpu.SemaphoreType.DMA, pltpu.VMEM
    far, held = pl.BlockSpec(memory_space=pltpu.HBM), pl.BlockSpec(memory_space=pltpu.VMEM)
    out = pl.pallas_call(
        functools.partial(section_kernel, Z),
        out_shape=jax.ShapeDtypeStruct((rows, D), bf16),
        in_specs=[far] * 11,
        out_specs=held,
        scratch_shapes=[
            V((rows, D), bf16), V(norm_gain.shape, f32), V(w_xbc.shape[1:], bf16),
            V((HEADS, KR), bf16), V(conv_weight.shape[1:], f32), V(conv_bias.shape, f32),
            V(dt_bias.shape, f32), V(dt_bias.shape, f32), V(dt_bias.shape, f32),
            V(inner_gain.shape, f32), V(w_out.shape[1:], bf16),
            V((Z, KR, CC), bf16), V((2 * Z * KR, CC), bf16),
            V((Z, 16, lanes), bf16), V((2 * Z, 16, lanes), bf16),
            V((VC, D), bf16),
            V((S, 2, rows, D), bf16), V((S, 2, rows, D), bf16),
            V((8 + rows, CC), f32), V((rows, CC), bf16), V((rows, VC), f32), V((STATE, VC), f32),
            V((S, 2, rows, D), bf16), V((S, 2, 8, rows), f32),
            V((S, 2, rows, D), bf16), V((S, 2, 8, rows), f32),
            V((2, rows, D), bf16), V((2, 8, rows), f32),
            V((S + 1, rows, D), bf16), V((S + 1, 8, rows), f32),
            V((rows, D), bf16),
            dma((11,)), dma((Z,)), dma((Z,)), dma((Z,)), dma((Z,)), dma((Z,)), dma((Z,)), dma((Z,)),
            dma((Z,)), dma, dma, dma((S, 2, 2)), dma((S, 2)), dma, dma((S, 2)), dma((S + 1,)),
            dma((S, 2)), dma((S + 1,)), dma((S, 2, 2)), dma((S, 2)), dma((2, 2)), dma((2,)), dma((2, 2)), dma((2,)), dma, dma,
        ],
        compiler_params=pltpu.CompilerParams(
            collective_id=0, has_side_effects=True, vmem_limit_bytes=67043328
        ),
    )(
        stream[0, 0], norm_gain, w_xbc[0], jnp.swapaxes(w_dt, 1, 2)[0], conv_weight[0], conv_bias,
        dt_bias, decay_rate, skip_weight, inner_gain, w_out[0],
    )
    return out[None, None]


def solution(mesh):
    placed = (
        P("section", "dp", "seq", None),
        P("section", None),
        P("section", ("seq", "dp"), None),
        P("section", ("seq", "dp"), None),
        P("section", None, None),
        P("section", None),
        P("section", None),
        P("section", None),
        P("section", None),
        P("section", None),
        P("section", ("seq", "dp"), None),
    )
    size = mesh.shape
    chips = size["dp"]
    whole_heads = HEADS % (2 * chips) == 0 and (INNER // chips) % 128 == 0
    body = fused if size["seq"] == 2 and chips == 4 and whole_heads and size["section"] > 1 else shards
    return jax.shard_map(
        body,
        mesh=mesh,
        in_specs=placed,
        out_specs=P("section", "dp", "seq", None),
        check_vma=False,
    )
```

```python
import functools

import jax
import jax.numpy as jnp
from jax import lax
from jax.experimental import pallas as pl
from jax.experimental.pallas import tpu as pltpu
from jax.sharding import PartitionSpec as P

HEADS = 40
HEAD_DIM = 64
STATE = 64
CONV = 4
BLOCK = 128
INNER = 2560


epsilon = 1e-05
QX = 4
QP = 4


def prefix(x, axis, combine, identity):
    devices, position = (lax.axis_size(axis), lax.axis_index(axis))
    everything = jax.tree.map(
        lambda part, kind: lax.all_gather(part.astype(kind), axis),
        x,
        jax.tree.map(lambda a: jnp.bfloat16 if a.dtype == jnp.float32 else a.dtype, x),
    )
    start = jax.tree.map(
        lambda part, zero: jnp.broadcast_to(jnp.asarray(zero, part.dtype), part.shape), x, identity
    )

    def hop(k, before):
        reached = k < position
        new = combine(
            before, jax.tree.map(lambda part, own: part[k].astype(own.dtype), everything, x)
        )
        return jax.tree.map(lambda a, b: jnp.where(reached, a, b), new, before)

    return lax.fori_loop(0, devices, hop, start)


def from_behind(x, axis, by):
    devices = lax.axis_size(axis)
    pairs = [(i, i + by) for i in range(devices) if 0 <= i + by < devices]
    return lax.ppermute(x, axis, pairs)


def passed_along(x, axis, by):
    devices = lax.axis_size(axis)
    return lax.ppermute(x, axis, [(i, (i + by) % devices) for i in range(devices)])


def rms_scale(values, scale_gain):
    mean_square = jnp.mean(values * values, axis=-1, keepdims=True)
    return values * lax.rsqrt(mean_square + epsilon) * scale_gain


def block_terms(values, b_rows, c_rows, dt_rows, head_rates):
    block_len = dt_rows.shape[0]
    cum_decay = jnp.cumsum(-dt_rows * head_rates[None, :], axis=0)
    scores = jnp.dot(c_rows, b_rows.T, preferred_element_type=jnp.float32)
    lag_decay = cum_decay.T[:, :, None] - cum_decay.T[:, None, :]
    causal = jnp.arange(block_len)[:, None] >= jnp.arange(block_len)[None, :]
    weights = jnp.where(causal[None], jnp.exp(jnp.minimum(lag_decay, 0.0)), 0.0)
    mixing = (scores[None] * weights * dt_rows.T[:, None, :]).astype(jnp.bfloat16)
    intra_out = jnp.einsum("hij,jhp->ihp", mixing, values, preferred_element_type=jnp.float32)
    tail_weight = jnp.exp(cum_decay[-1][None, :] - cum_decay) * dt_rows
    scaled = (values.astype(jnp.float32) * tail_weight[:, :, None]).astype(jnp.bfloat16)
    summary = jnp.einsum("jhp,jn->hpn", scaled, b_rows, preferred_element_type=jnp.float32)
    return (intra_out, summary, jnp.exp(cum_decay[-1]), jnp.exp(cum_decay))


def state_output(c_rows, growth, carried):
    readout = jnp.einsum(
        "in,hpn->ihp", c_rows.astype(jnp.float32), carried, precision=lax.Precision.HIGHEST
    )
    return growth[:, :, None] * readout


def combine_states(earlier, latest):
    decay_a, state_a = earlier
    decay_b, state_b = latest
    return (decay_a * decay_b, decay_b[:, None] * state_a + state_b)


def chain_states(summary):
    identity = (jnp.ones_like(summary[0]), jnp.zeros_like(summary[1]))
    return prefix(summary, "seq", combine_states, identity)


def project_rows(normed_rows, xbc_part, dt_part):
    return (
        jnp.dot(
            normed_rows,
            lax.all_gather(xbc_part, ("seq", "dp"), axis=0, tiled=True),
            preferred_element_type=jnp.float32,
        ),
        jnp.dot(
            normed_rows,
            lax.all_gather(dt_part, ("seq", "dp"), axis=0, tiled=True),
            preferred_element_type=jnp.float32,
        ),
    )


def shards(
    stream,
    norm_gain,
    w_xbc,
    w_dt,
    conv_weight,
    conv_bias,
    dt_bias,
    decay_rate,
    skip_weight,
    inner_gain,
    w_out,
):
    rows_in = stream[0, 0]
    length_dev = rows_in.shape[0]
    margin = CONV - 1
    row_gain = norm_gain[0]
    normed = rms_scale(rows_in.astype(jnp.float32), row_gain).astype(jnp.bfloat16)
    projected, dt_raw = project_rows(normed, w_xbc[0], w_dt[0])
    xbc_raw = projected.astype(jnp.bfloat16)
    prev_proj = from_behind(xbc_raw[length_dev - margin :], "seq", 1)
    padded = jnp.concatenate([prev_proj, xbc_raw], axis=0)
    conv_sum = jnp.broadcast_to(conv_bias[0][None, :], (length_dev, padded.shape[1]))
    for tap_index in range(CONV):
        conv_sum = conv_sum + conv_weight[0, tap_index][None, :] * padded[
            tap_index : tap_index + length_dev
        ].astype(jnp.float32)
    mixed_rows = jax.nn.silu(conv_sum).astype(jnp.bfloat16)
    blocks = length_dev // BLOCK
    values = mixed_rows[:, :INNER].reshape(blocks, BLOCK, HEADS, HEAD_DIM)
    b_rows = mixed_rows[:, INNER : INNER + STATE].reshape(blocks, BLOCK, STATE)
    c_rows = mixed_rows[:, INNER + STATE :].reshape(blocks, BLOCK, STATE)
    dt_rows = jax.nn.softplus(dt_raw + dt_bias[0][None, :]).reshape(blocks, BLOCK, HEADS)
    intra_out, summary, totals, growth = jax.vmap(block_terms, in_axes=(0, 0, 0, 0, None))(
        values, b_rows, c_rows, dt_rows, decay_rate[0]
    )

    def local_step(running, inputs):
        carried, decay_before = running
        block_total, block_summary = inputs
        return (
            (block_total[:, None, None] * carried + block_summary, decay_before * block_total),
            (carried, decay_before),
        )

    start_state = (
        jnp.zeros((HEADS, HEAD_DIM, STATE), jnp.float32),
        jnp.ones((HEADS,), jnp.float32),
    )
    (local_state, local_decay), (enter_local, decay_before) = lax.scan(
        local_step, start_state, (totals, summary)
    )
    state_terms = jax.vmap(state_output)
    early_terms = state_terms(c_rows, growth, enter_local)
    incoming_decay, incoming_flat = chain_states(
        (local_decay, local_state.reshape(HEADS, HEAD_DIM * STATE))
    )
    arriving = incoming_flat.reshape(HEADS, HEAD_DIM, STATE)
    late_terms = state_terms(c_rows, growth, decay_before[:, :, None, None] * arriving[None])
    state_part = early_terms + late_terms
    mixed_out = (
        intra_out + state_part + skip_weight[0][None, None, :, None] * values.astype(jnp.float32)
    )
    normed_out = rms_scale(mixed_out.reshape(length_dev, INNER), inner_gain[0]).astype(jnp.bfloat16)
    branch_out = jnp.dot(
        normed_out,
        lax.all_gather(w_out[0], ("seq", "dp"), axis=0, tiled=True),
        preferred_element_type=jnp.float32,
    )
    next_rows = (rows_in.astype(jnp.float32) + branch_out).astype(jnp.bfloat16)
    shifted = passed_along(next_rows, "section", 1)
    return shifted[None, None]

def section_kernel(
    Z, x_hbm, ng_hbm, w_hbm, wd_hbm, cw_hbm, cb_hbm, db_hbm, dr_hbm, sk_hbm, ig_hbm, wo_hbm,
    out_ref,
    x_ref, ng_ref, w_ref, wd_ref, cw_ref, cb_ref, db_ref, dr_ref, sk_ref, ig_ref, wo_ref, w2,
    wbuf, d2, dbuf, wobuf, sbuf, nbuf, cbuf, tails, vbuf, ybuf, state,
    pbuf, stbuf, xpart, xstat, bpart, bstat, rpart, rstat, obuf,
    l_sem, w_send, w_recv, d_send, d_recv, f_send, f_recv, g_send, g_recv, o_send, o_recv,
    i_send, s_send, s_recv, e_send, e_recv, p_send, p_recv, t_send, t_recv,
    q_send, x_recv, y_recv, b_send, c_send,
):
    z = lax.axis_index("dp")
    c = lax.axis_index("seq")
    sec = lax.axis_index("section")
    NS = lax.axis_size("section")
    nxt = lax.rem(sec + 1, NS)
    prv = lax.rem(sec + NS - 1, NS)
    S = Z // 2
    rows, D = x_ref.shape
    KR = w_ref.shape[0]
    per = INNER // (2 * Z)
    hper = HEADS // (2 * Z)
    VC = 2 * per
    NB = 2 * STATE
    CC = VC + NB
    f32, bf16 = jnp.float32, jnp.bfloat16
    core = lax.rem(z, 2)
    own_core = core == c
    myslot = z // 2
    sib = {"seq": 1 - c}
    upper = z >= S
    border = jnp.where(upper, S, S - 1)
    edge = jnp.where(upper, Z - 1, 0)
    near = jnp.where(upper, S - 1, 0)
    far = 1 - near
    scope = jax.named_scope

    def rcopy(src, dst, ss, rs, where):
        return pltpu.make_async_remote_copy(
            src_ref=src, dst_ref=dst, send_sem=ss, recv_sem=rs, device_id=where,
            device_id_type=pl.DeviceIdType.MESH,
        )

    def band(q, parts):
        return pl.ds(q * (rows // parts), rows // parts)

    loads = [
        pltpu.make_async_copy(src, dst, l_sem.at[i])
        for i, (src, dst) in enumerate((
            (x_hbm, x_ref), (w_hbm, w_ref), (wd_hbm, wd_ref), (wo_hbm, wo_ref), (ng_hbm, ng_ref),
            (cw_hbm, cw_ref), (cb_hbm, cb_ref), (db_hbm, db_ref), (dr_hbm, dr_ref), (sk_hbm, sk_ref),
            (ig_hbm, ig_ref)))
    ]
    for load in loads:
        load.start()
    barrier = pltpu.get_barrier_semaphore()
    for d in range(Z):
        for e in range(2):
            @pl.when(jnp.logical_not(jnp.logical_and(d == z, e == c)))
            def _():
                pl.semaphore_signal(barrier, inc=1, device_id={"dp": d, "seq": e},
                                    device_id_type=pl.DeviceIdType.MESH)
    for s in (nxt, prv):
        pl.semaphore_signal(barrier, inc=1, device_id={"section": s},
                            device_id_type=pl.DeviceIdType.MESH)

    def row0(core, chip):
        return pl.multiple_of((core * Z + chip) * KR, KR)

    lanes = d2.shape[2]
    loads[2].wait()
    for d in range(Z):
        two = jnp.concatenate(
            [wd_ref[d * hper : (d + 1) * hper, :].astype(f32),
             wd_ref[(Z + d) * hper : (Z + d + 1) * hper, :].astype(f32),
             jnp.zeros((16 - 2 * hper, KR), f32)], axis=0)
        d2[d] = jnp.concatenate([two, jnp.zeros((16, lanes - KR), f32)], axis=1).astype(bf16)
    dbuf[c * Z + z] = d2[z]
    loads[0].wait()
    loads[1].wait()
    for d in range(Z):
        w2[d, :, 0:per] = w_ref[:, d * per : (d + 1) * per]
        w2[d, :, per:VC] = w_ref[:, Z * per + d * per : Z * per + (d + 1) * per]
        w2[d, :, VC:CC] = w_ref[:, INNER : INNER + NB]

    with scope("barrier"):
        pl.semaphore_wait(barrier, 2 * Z - 1 + 2)

    def i_copy(q, way):
        where = sib if way == 0 else {"dp": z + (1 if way == 1 else -1), "seq": core}
        at = band(q, QX)
        return rcopy(x_ref.at[at], sbuf.at[myslot, c, at], i_send.at[way, q], s_recv.at[myslot, c, q], where)

    ways = ((0, jnp.logical_not(own_core)), (1, z + 1 < Z), (2, z > 0))

    def send_x(on, inward):
        for way, there in ways[1:]:
            towards = jnp.logical_xor(upper, way == 1)
            @pl.when(jnp.logical_and(jnp.logical_and(on, there), towards if inward else jnp.logical_not(towards)))
            def _():
                for q in range(QX):
                    i_copy(q, way).start()

    def s_copy(k, h, q, up):
        at = band(q, QX)
        return rcopy(sbuf.at[k, h, at], sbuf.at[k, h, at], s_send.at[k, h, q], s_recv.at[k, h, q],
                     {"dp": z + (1 if up else -1)})

    def relay(k, h, q, fn):
        b = 2 * k + c
        @pl.when(jnp.logical_and(z > b, z + 1 < Z))
        def _():
            fn(s_copy(k, h, q, True))
        @pl.when(jnp.logical_and(z < b, z > 0))
        def _():
            fn(s_copy(k, h, q, False))

    def pass_on(k, h, chunks=range(QX)):
        for q in chunks:
            @pl.when(jnp.logical_not(jnp.logical_and(own_core, jnp.logical_and(k == myslot, h == c))))
            def _():
                s_copy(k, h, q, True).wait_recv()
            relay(k, h, q, lambda cp: cp.start())

    inner = z == border
    outer = z != border

    def pass_at(k, h, on, chunks=range(QX)):
        @pl.when(on)
        def _():
            pass_on(k, h, chunks)

    one, two = jnp.where(inner, far, near), jnp.where(inner, near, far)

    def w_copies(d, frm):
        at = pl.ds(row0(c, frm), KR)
        g = c * Z + frm
        return (rcopy(w2.at[d], wbuf.at[at], w_send.at[d], w_recv.at[frm], {"dp": d}),
                rcopy(d2.at[d], dbuf.at[g], d_send.at[d], d_recv.at[frm], {"dp": d}))

    def f_copies(d, core):
        at = pl.ds(row0(core, d), KR)
        g = core * Z + d
        return (rcopy(wbuf.at[at], wbuf.at[at], f_send.at[d], f_recv.at[d], sib),
                rcopy(dbuf.at[g], dbuf.at[g], g_send.at[d], g_recv.at[d], sib))

    def send_w(d, on):
        @pl.when(on)
        def _():
            for cp in w_copies(d, z):
                cp.start()

    @pl.when(ways[0][1])
    def _():
        for q in range(QX):
            i_copy(q, 0).start()
    own_fwd = (
        rcopy(w2.at[z], wbuf.at[pl.ds(row0(c, z), KR)], f_send.at[z], f_recv.at[z], sib),
        rcopy(d2.at[z], dbuf.at[c * Z + z], g_send.at[z], g_recv.at[z], sib),
    )
    for cp in own_fwd:
        cp.start()
    wbuf[pl.ds(row0(c, z), KR), :] = w2[z]

    @pl.when(own_core)
    def _():
        sbuf[myslot, c] = x_ref[...]

    with scope("early"):
        send_x(c == 0, True)
        send_x(c == 0, False)
        send_w(jnp.where(upper, 0, Z - 1), inner)
        send_w(edge, inner)
        for step in (3, 1, 2):
            send_w(jnp.where(upper, z - step, z + step), outer)
        pass_at(near, 0, inner)
        send_w(jnp.where(upper, S - 1, S), inner)
        send_x(jnp.logical_and(c == 1, outer), True)

    loads[3].wait()
    at_wo = pl.ds(pl.multiple_of(c * per, per), per)
    wo_copy = rcopy(wo_ref, wobuf.at[at_wo], o_send, o_recv, sib)
    wo_copy.start()
    wobuf[at_wo, :] = wo_ref[...]
    for load in loads[4:]:
        load.wait()

    def pick(ref, width, tail):
        wide = Z * width
        got = None
        for d in range(Z):
            part = jnp.concatenate(
                [ref[:, d * width : (d + 1) * width],
                 ref[:, wide + d * width : wide + (d + 1) * width]], axis=1)
            part = jnp.where(z == d, part, 0.0)
            got = part if got is None else got + part
        return jnp.concatenate([got, tail], axis=1) if tail is not None else got

    gain_in = ng_ref[...]
    hi = lax.Precision.HIGHEST
    taps = pick(cw_ref, per, cw_ref[:, INNER : INNER + NB])
    tbias = pick(cb_ref, per, cb_ref[:, INNER : INNER + NB])
    hz = jnp.zeros((1, 128 - 2 * hper), f32)
    heads = jnp.concatenate(
        [pick(db_ref, hper, hz), pick(dr_ref, hper, hz), pick(sk_ref, hper, hz),
         jnp.zeros((5, 128), f32)], axis=0)
    heads_t = heads.T[0:16]
    dtb, rate = heads_t[:, 0:1], heads_t[:, 1:2]
    gain_out = pick(ig_ref, per, None)
    spread = (lax.broadcasted_iota(jnp.int32, (16, VC), 1) // HEAD_DIM
              == lax.broadcasted_iota(jnp.int32, (16, VC), 0)).astype(f32)

    def widen(m):
        return jnp.dot(m, spread, precision=hi, preferred_element_type=f32)

    skip_wide = widen(heads[:, 0:16])[2:3]
    ii = lax.broadcasted_iota(jnp.int32, (BLOCK, BLOCK), 0)
    jj = lax.broadcasted_iota(jnp.int32, (BLOCK, BLOCK), 1)
    causal = ii >= jj
    triu = (ii <= jj).astype(f32)
    low_lane = lax.broadcasted_iota(jnp.int32, (BLOCK, 128), 1) < HEAD_DIM
    margin = CONV - 1

    def norm_in(k, h):
        v = sbuf[k, h].astype(f32)
        ms = jnp.mean(v * v, axis=-1, keepdims=True)
        nbuf[k, h] = (v * lax.rsqrt(ms + epsilon) * gain_in).astype(bf16)

    def unit(k, h, hook=None):
        nb = nbuf[k, h]
        if h == 0:
            cbuf[0:8, :] = jnp.zeros((8, CC), f32)
        else:
            cbuf[0:8, :] = tails[k]
        cbuf[8 : 8 + rows, :] = jnp.dot(nb, wbuf[...], preferred_element_type=f32).astype(bf16).astype(f32)
        if h == 0:
            tails[k] = cbuf[rows : rows + 8, :]
        acc = jnp.broadcast_to(tbias, (rows, CC))
        for t in range(CONV):
            acc = acc + taps[t : t + 1, :] * cbuf[8 - margin + t : 8 - margin + t + rows, :]
        vbuf[...] = (acc / (1.0 + jnp.exp(-acc))).astype(bf16)
        if hook is not None:
            hook()
        raw = lax.dot_general(w_steps, nb, (((1,), (1,)), ((), ())), preferred_element_type=f32) + dtb
        dt_t = jnp.maximum(raw, 0.0) + jnp.log1p(jnp.exp(-jnp.abs(raw)))
        cum_t = jnp.dot(-dt_t * rate, triu, precision=hi, preferred_element_type=f32)
        tail_t = jnp.exp(cum_t[:, BLOCK - 1 : BLOCK] - cum_t) * dt_t
        cols = jnp.concatenate([cum_t, tail_t, jnp.exp(cum_t), jnp.zeros((80, BLOCK), f32)], axis=0).T
        cum = cols[:, 0:16]
        bm = vbuf[:, VC : VC + STATE]
        cm = vbuf[:, VC + STATE : CC]
        scores = lax.dot_general(cm, bm, (((1,), (1,)), ((), ())), preferred_element_type=f32)
        scores = jnp.where(causal, scores, 0.0)
        vals = vbuf[:, 0:VC].astype(f32)
        part = skip_wide * vals
        if h > 0:
            grow = widen(cols[:, 32:48])
            part = part + grow * jnp.dot(cm.astype(f32), state[k], precision=hi,
                                         preferred_element_type=f32)
        for p in range(VC // 128):
            mix = []
            for q in range(2):
                hd = 2 * p + q
                lag = cum[:, hd : hd + 1] - cum_t[hd : hd + 1, :]
                m = scores * jnp.exp(jnp.minimum(lag, 0.0)) * dt_t[hd : hd + 1, :]
                mix.append(m.astype(bf16))
            vp = vals[:, p * 128 : (p + 1) * 128]
            two = jnp.concatenate([jnp.where(low_lane, vp, 0.0), jnp.where(low_lane, 0.0, vp)],
                                  axis=0).astype(bf16)
            got = jnp.dot(jnp.concatenate(mix, axis=1), two, preferred_element_type=f32)
            ybuf[:, p * 128 : (p + 1) * 128] = got + part[:, p * 128 : (p + 1) * 128]
        y = ybuf[...]
        pbuf[k, h] = jnp.dot((y * gain_out).astype(bf16), wobuf[...], preferred_element_type=f32).astype(bf16)
        stbuf[k, h] = lax.dot_general(jnp.ones((8, VC), f32), y * y, (((1,), (1,)), ((), ())),
                                      precision=hi, preferred_element_type=f32)
        if h == 0:
            scaled = (vals * widen(cols[:, 16:32])).astype(bf16)
            state[k] = lax.dot_general(bm, scaled, (((0,), (0,)), ((), ())), preferred_element_type=f32)

    def place(b, h):
        return {"dp": b, "seq": h}

    def here(h):
        return jnp.logical_and(own_core, h == c)

    def p_copies(h):
        slot = lax.rem(z, S)
        where = place(2 * near + c, h)
        return (rcopy(stbuf.at[near, h], rstat.at[slot], t_send.at[near, h], t_recv.at[slot], where),
                *(rcopy(pbuf.at[near, h, band(q, QP)], rpart.at[slot, band(q, QP)], p_send.at[h, q],
                        p_recv.at[slot, q], where) for q in range(QP)))

    def x_copies(h, q):
        at = band(q, QP)
        big = rcopy(pbuf.at[far, h, at], xpart.at[h, at], q_send.at[h, q], x_recv.at[h, q], {"dp": border})
        if q > 0:
            return (big,)
        return (rcopy(stbuf.at[far, h], xstat.at[h], t_send.at[far, h], y_recv.at[h], {"dp": border}), big)

    def b_copies(h, q):
        where = place(2 * far + c, h)
        at = band(q, QP)
        big = rcopy(bpart.at[h, at], rpart.at[S, at], b_send.at[h, q], p_recv.at[S, q], where)
        if q > 0:
            return (big,)
        return (rcopy(bstat.at[h], rstat.at[S], c_send.at[h], t_recv.at[S], where), big)

    def send_far(h):
        @pl.when(outer)
        def _():
            for q in range(QP):
                for cp in x_copies(h, q):
                    cp.start()

    def send_near(h, now):
        @pl.when(jnp.logical_and(now, here(h)))
        def _():
            rpart[lax.rem(z, S)] = pbuf[near, h]
            rstat[lax.rem(z, S)] = stbuf[near, h]

        @pl.when(jnp.logical_and(now, jnp.logical_not(here(h))))
        def _():
            for cp in p_copies(h):
                cp.start()

    def sum_far(h):
        @pl.when(z == border)
        def _():
            for q in range(QP):
                at = band(q, QP)
                for cp in x_copies(h, q):
                    cp.wait_recv()
                bpart[h, at] = (pbuf[far, h, at].astype(f32) + xpart[h, at].astype(f32)).astype(bf16)
                if q == 0:
                    bstat[h] = stbuf[far, h] + xstat[h]
                for cp in b_copies(h, q):
                    cp.start()

    with scope("passf0i"):
        pass_at(far, 0, inner)
    send_x(jnp.logical_and(c == 1, inner), True)
    for step in range(1, Z):
        for d in (z + step, z - step):
            @pl.when(jnp.logical_and(d >= 0, d < Z))
            def _():
                with scope(f"wrecv{step}"):
                    for cp in w_copies(z, d):
                        cp.wait_recv()
                for cp in f_copies(d, c):
                    cp.start()
    with scope("passn1i"):
        pass_at(near, 1, inner)
    with scope("fwait"):
        for d in range(Z):
            for cp in f_copies(d, 1 - c):
                cp.wait_recv()
        wo_copy.wait_recv()
    w_steps = jnp.concatenate([dbuf[g][:, 0:KR].astype(f32) for g in range(2 * Z)], axis=1).astype(bf16)

    with scope("passf1h"):
        None
    with scope("passn0"):
        pass_at(near, 0, outer)
    with scope("unit0"):
        norm_in(one, 0)
        unit(one, 0, lambda: pass_at(far, 1, inner, (0,)))
    send_near(0, outer)
    with scope("passf1i"):
        pass_at(far, 1, inner, (1,))
    with scope("passf0"):
        pass_at(far, 0, outer)
    with scope("unit1"):
        norm_in(two, 0)
        unit(two, 0, lambda: pass_at(far, 1, inner, (2,)))
    send_far(0)
    with scope("passf1j"):
        pass_at(far, 1, inner, (3,))
    send_x(jnp.logical_and(c == 1, inner), False)
    with scope("passf1"):
        pass_at(far, 1, outer)
    with scope("unit2"):
        norm_in(two, 1)
        unit(two, 1)
    send_far(1)
    with scope("sumf0"):
        sum_far(0)
    with scope("passn1"):
        pass_at(near, 1, outer)
    with scope("unit3"):
        norm_in(one, 1)
        unit(one, 1)
    for h in range(2):
        send_near(h, inner)
    send_near(1, outer)
    with scope("sumf1"):
        sum_far(1)
    def r_copies(j, q):
        at = band(q, QP)
        big = rcopy(pbuf.at[0, 0, at], rpart.at[j, at], p_send.at[0, q], p_recv.at[j, q], sib)
        if q > 0:
            return (big,)
        return (rcopy(stbuf.at[0, 0], rstat.at[j], t_send.at[0, 0], t_recv.at[j], sib), big)

    def e_copy(q):
        at = band(q, QP)
        return rcopy(obuf.at[at], out_ref.at[at], e_send.at[q], e_recv.at[q], {"section": nxt})

    scale = None
    for q in range(QP):
        at = band(q, QP)
        with scope(f"rwait{q}"):
            for j in range(S + 1):
                mine = jnp.logical_and(own_core, lax.rem(z, S) == j) if j < S else False
                @pl.when(jnp.logical_not(mine))
                def _():
                    for cp in r_copies(j, q):
                        cp.wait_recv()
        if q == 0:
            stat = rstat[0]
            for j in range(1, S + 1):
                stat = stat + rstat[j]
            scale = lax.rsqrt(stat * (1.0 / INNER) + epsilon).T[:, 0:1]
        total = rpart[0, at].astype(f32)
        for j in range(1, S + 1):
            total = total + rpart[j, at].astype(f32)
        size = rows // QP
        obuf[at, :] = (x_ref[at].astype(f32) + total * scale[q * size : (q + 1) * size]).astype(bf16)
        e_copy(q).start()

    with scope("sends"):
        for q in range(QX):
            for way, on in ways:
                @pl.when(on)
                def _():
                    i_copy(q, way).wait_send()
        for cp in (*own_fwd, wo_copy):
            cp.wait_send()
        for d in range(Z):
            @pl.when(d != z)
            def _():
                for cp in (*w_copies(d, z), *f_copies(d, c)):
                    cp.wait_send()
        for h in range(2):
            for q in range(QX):
                for k in range(S):
                    relay(k, h, q, lambda cp: cp.wait_send())
            for q in range(QP):
                @pl.when(z != border)
                def _():
                    for cp in x_copies(h, q):
                        cp.wait_send()
                @pl.when(z == border)
                def _():
                    for cp in b_copies(h, q):
                        cp.wait_send()
            @pl.when(jnp.logical_not(here(h)))
            def _():
                for cp in p_copies(h):
                    cp.wait_send()
    with scope("last"):
        for q in range(QP):
            e_copy(q).wait()


def fused(
    stream, norm_gain, w_xbc, w_dt, conv_weight, conv_bias, dt_bias, decay_rate, skip_weight,
    inner_gain, w_out,
):
    Z = lax.axis_size("dp")
    rows, D = stream.shape[2:]
    if rows != BLOCK:
        return shards(stream, norm_gain, w_xbc, w_dt, conv_weight, conv_bias, dt_bias, decay_rate,
                      skip_weight, inner_gain, w_out)
    KR = w_xbc.shape[1]
    VC = INNER // Z
    CC = VC + 2 * STATE
    S = Z // 2
    lanes = -(-KR // 128) * 128
    bf16, f32 = jnp.bfloat16, jnp.float32
    dma, V = pltpu.SemaphoreType.DMA, pltpu.VMEM
    far, held = pl.BlockSpec(memory_space=pltpu.HBM), pl.BlockSpec(memory_space=pltpu.VMEM)
    out = pl.pallas_call(
        functools.partial(section_kernel, Z),
        out_shape=jax.ShapeDtypeStruct((rows, D), bf16),
        in_specs=[far] * 11,
        out_specs=held,
        scratch_shapes=[
            V((rows, D), bf16), V(norm_gain.shape, f32), V(w_xbc.shape[1:], bf16),
            V((HEADS, KR), bf16), V(conv_weight.shape[1:], f32), V(conv_bias.shape, f32),
            V(dt_bias.shape, f32), V(dt_bias.shape, f32), V(dt_bias.shape, f32),
            V(inner_gain.shape, f32), V(w_out.shape[1:], bf16),
            V((Z, KR, CC), bf16), V((2 * Z * KR, CC), bf16),
            V((Z, 16, lanes), bf16), V((2 * Z, 16, lanes), bf16),
            V((VC, D), bf16),
            V((S, 2, rows, D), bf16), V((S, 2, rows, D), bf16),
            V((8 + rows, CC), f32), V((S, 8, CC), f32), V((rows, CC), bf16), V((rows, VC), f32),
            V((S, STATE, VC), f32),
            V((S, 2, rows, D), bf16), V((S, 2, 8, rows), f32),
            V((2, rows, D), bf16), V((2, 8, rows), f32),
            V((2, rows, D), bf16), V((2, 8, rows), f32),
            V((S + 1, rows, D), bf16), V((S + 1, 8, rows), f32),
            V((rows, D), bf16),
            dma((11,)), dma((Z,)), dma((Z,)), dma((Z,)), dma((Z,)), dma((Z,)), dma((Z,)), dma((Z,)),
            dma((Z,)), dma, dma,
            dma((3, QX)), dma((S, 2, QX)), dma((S, 2, QX)), dma((QP,)), dma((QP,)), dma((2, QP)), dma((S + 1, QP)),
            dma((S, 2)), dma((S + 1,)),
            dma((2, QP)), dma((2, QP)), dma((2,)), dma((2, QP)), dma((2,)),
        ],
        compiler_params=pltpu.CompilerParams(
            collective_id=0, has_side_effects=True, vmem_limit_bytes=50 * 1024 * 1024
        ),
    )(
        *(pltpu.with_memory_space_constraint(a, pltpu.HBM) for a in (
            stream[0, 0], norm_gain, w_xbc[0], jnp.swapaxes(w_dt, 1, 2)[0], conv_weight[0], conv_bias,
            dt_bias, decay_rate, skip_weight, inner_gain, w_out[0]))
    )
    return out[None, None]


def solution(mesh):
    placed = (
        P("section", "dp", "seq", None),
        P("section", None),
        P("section", ("seq", "dp"), None),
        P("section", ("seq", "dp"), None),
        P("section", None, None),
        P("section", None),
        P("section", None),
        P("section", None),
        P("section", None),
        P("section", None),
        P("section", ("seq", "dp"), None),
    )
    size = mesh.shape
    chips = size["dp"]
    whole_heads = HEADS % (2 * chips) == 0 and (INNER // chips) % 128 == 0
    body = fused if size["seq"] == 2 and chips == 4 and whole_heads and size["section"] > 1 else shards
    return jax.shard_map(
        body,
        mesh=mesh,
        in_specs=placed,
        out_specs=P("section", "dp", "seq", None),
        check_vma=False,
    )
```

```python
import functools

import jax
import jax.numpy as jnp
from jax import lax
from jax.experimental import pallas as pl
from jax.experimental.pallas import tpu as pltpu
from jax.sharding import PartitionSpec as P

HEADS = 40
HEAD_DIM = 64
STATE = 64
CONV = 4
BLOCK = 128
INNER = 2560


epsilon = 1e-05
QX = 4
QP = 4


def prefix(x, axis, combine, identity):
    devices, position = (lax.axis_size(axis), lax.axis_index(axis))
    everything = jax.tree.map(
        lambda part, kind: lax.all_gather(part.astype(kind), axis),
        x,
        jax.tree.map(lambda a: jnp.bfloat16 if a.dtype == jnp.float32 else a.dtype, x),
    )
    start = jax.tree.map(
        lambda part, zero: jnp.broadcast_to(jnp.asarray(zero, part.dtype), part.shape), x, identity
    )

    def hop(k, before):
        reached = k < position
        new = combine(
            before, jax.tree.map(lambda part, own: part[k].astype(own.dtype), everything, x)
        )
        return jax.tree.map(lambda a, b: jnp.where(reached, a, b), new, before)

    return lax.fori_loop(0, devices, hop, start)


def from_behind(x, axis, by):
    devices = lax.axis_size(axis)
    pairs = [(i, i + by) for i in range(devices) if 0 <= i + by < devices]
    return lax.ppermute(x, axis, pairs)


def passed_along(x, axis, by):
    devices = lax.axis_size(axis)
    return lax.ppermute(x, axis, [(i, (i + by) % devices) for i in range(devices)])


def rms_scale(values, scale_gain):
    mean_square = jnp.mean(values * values, axis=-1, keepdims=True)
    return values * lax.rsqrt(mean_square + epsilon) * scale_gain


def block_terms(values, b_rows, c_rows, dt_rows, head_rates):
    block_len = dt_rows.shape[0]
    cum_decay = jnp.cumsum(-dt_rows * head_rates[None, :], axis=0)
    scores = jnp.dot(c_rows, b_rows.T, preferred_element_type=jnp.float32)
    lag_decay = cum_decay.T[:, :, None] - cum_decay.T[:, None, :]
    causal = jnp.arange(block_len)[:, None] >= jnp.arange(block_len)[None, :]
    weights = jnp.where(causal[None], jnp.exp(jnp.minimum(lag_decay, 0.0)), 0.0)
    mixing = (scores[None] * weights * dt_rows.T[:, None, :]).astype(jnp.bfloat16)
    intra_out = jnp.einsum("hij,jhp->ihp", mixing, values, preferred_element_type=jnp.float32)
    tail_weight = jnp.exp(cum_decay[-1][None, :] - cum_decay) * dt_rows
    scaled = (values.astype(jnp.float32) * tail_weight[:, :, None]).astype(jnp.bfloat16)
    summary = jnp.einsum("jhp,jn->hpn", scaled, b_rows, preferred_element_type=jnp.float32)
    return (intra_out, summary, jnp.exp(cum_decay[-1]), jnp.exp(cum_decay))


def state_output(c_rows, growth, carried):
    readout = jnp.einsum(
        "in,hpn->ihp", c_rows.astype(jnp.float32), carried, precision=lax.Precision.HIGHEST
    )
    return growth[:, :, None] * readout


def combine_states(earlier, latest):
    decay_a, state_a = earlier
    decay_b, state_b = latest
    return (decay_a * decay_b, decay_b[:, None] * state_a + state_b)


def chain_states(summary):
    identity = (jnp.ones_like(summary[0]), jnp.zeros_like(summary[1]))
    return prefix(summary, "seq", combine_states, identity)


def project_rows(normed_rows, xbc_part, dt_part):
    return (
        jnp.dot(
            normed_rows,
            lax.all_gather(xbc_part, ("seq", "dp"), axis=0, tiled=True),
            preferred_element_type=jnp.float32,
        ),
        jnp.dot(
            normed_rows,
            lax.all_gather(dt_part, ("seq", "dp"), axis=0, tiled=True),
            preferred_element_type=jnp.float32,
        ),
    )


def shards(
    stream,
    norm_gain,
    w_xbc,
    w_dt,
    conv_weight,
    conv_bias,
    dt_bias,
    decay_rate,
    skip_weight,
    inner_gain,
    w_out,
):
    rows_in = stream[0, 0]
    length_dev = rows_in.shape[0]
    margin = CONV - 1
    row_gain = norm_gain[0]
    normed = rms_scale(rows_in.astype(jnp.float32), row_gain).astype(jnp.bfloat16)
    projected, dt_raw = project_rows(normed, w_xbc[0], w_dt[0])
    xbc_raw = projected.astype(jnp.bfloat16)
    prev_proj = from_behind(xbc_raw[length_dev - margin :], "seq", 1)
    padded = jnp.concatenate([prev_proj, xbc_raw], axis=0)
    conv_sum = jnp.broadcast_to(conv_bias[0][None, :], (length_dev, padded.shape[1]))
    for tap_index in range(CONV):
        conv_sum = conv_sum + conv_weight[0, tap_index][None, :] * padded[
            tap_index : tap_index + length_dev
        ].astype(jnp.float32)
    mixed_rows = jax.nn.silu(conv_sum).astype(jnp.bfloat16)
    blocks = length_dev // BLOCK
    values = mixed_rows[:, :INNER].reshape(blocks, BLOCK, HEADS, HEAD_DIM)
    b_rows = mixed_rows[:, INNER : INNER + STATE].reshape(blocks, BLOCK, STATE)
    c_rows = mixed_rows[:, INNER + STATE :].reshape(blocks, BLOCK, STATE)
    dt_rows = jax.nn.softplus(dt_raw + dt_bias[0][None, :]).reshape(blocks, BLOCK, HEADS)
    intra_out, summary, totals, growth = jax.vmap(block_terms, in_axes=(0, 0, 0, 0, None))(
        values, b_rows, c_rows, dt_rows, decay_rate[0]
    )

    def local_step(running, inputs):
        carried, decay_before = running
        block_total, block_summary = inputs
        return (
            (block_total[:, None, None] * carried + block_summary, decay_before * block_total),
            (carried, decay_before),
        )

    start_state = (
        jnp.zeros((HEADS, HEAD_DIM, STATE), jnp.float32),
        jnp.ones((HEADS,), jnp.float32),
    )
    (local_state, local_decay), (enter_local, decay_before) = lax.scan(
        local_step, start_state, (totals, summary)
    )
    state_terms = jax.vmap(state_output)
    early_terms = state_terms(c_rows, growth, enter_local)
    incoming_decay, incoming_flat = chain_states(
        (local_decay, local_state.reshape(HEADS, HEAD_DIM * STATE))
    )
    arriving = incoming_flat.reshape(HEADS, HEAD_DIM, STATE)
    late_terms = state_terms(c_rows, growth, decay_before[:, :, None, None] * arriving[None])
    state_part = early_terms + late_terms
    mixed_out = (
        intra_out + state_part + skip_weight[0][None, None, :, None] * values.astype(jnp.float32)
    )
    normed_out = rms_scale(mixed_out.reshape(length_dev, INNER), inner_gain[0]).astype(jnp.bfloat16)
    branch_out = jnp.dot(
        normed_out,
        lax.all_gather(w_out[0], ("seq", "dp"), axis=0, tiled=True),
        preferred_element_type=jnp.float32,
    )
    next_rows = (rows_in.astype(jnp.float32) + branch_out).astype(jnp.bfloat16)
    shifted = passed_along(next_rows, "section", 1)
    return shifted[None, None]

def section_kernel(
    Z, x_hbm, ng_hbm, w_hbm, wd_hbm, cw_hbm, cb_hbm, db_hbm, dr_hbm, sk_hbm, ig_hbm, wo_hbm,
    out_ref,
    x_ref, ng_ref, w_ref, wd_ref, cw_ref, cb_ref, db_ref, dr_ref, sk_ref, ig_ref, wo_ref, w2,
    wbuf, d2, dbuf, wobuf, sbuf, nbuf, cbuf, tails, vbuf, ybuf, state,
    pbuf, stbuf, xpart, xstat, bpart, bstat, kpart, kstat, jpart, jstat, rpart, rstat, obuf,
    l_sem, w_send, w_recv, d_send, d_recv, f_send, f_recv, g_send, g_recv, o_send, o_recv,
    i_send, s_send, s_recv, e_send, e_recv, p_send, p_recv, t_send, t_recv,
    q_send, x_recv, y_recv, b_send, c_send, k_recv, kt_recv, j_send, jt_send,
):
    z = lax.axis_index("dp")
    c = lax.axis_index("seq")
    sec = lax.axis_index("section")
    NS = lax.axis_size("section")
    nxt = lax.rem(sec + 1, NS)
    prv = lax.rem(sec + NS - 1, NS)
    S = Z // 2
    rows, D = x_ref.shape
    KR = w_ref.shape[0]
    per = INNER // (2 * Z)
    hper = HEADS // (2 * Z)
    VC = 2 * per
    NB = 2 * STATE
    CC = VC + NB
    f32, bf16 = jnp.float32, jnp.bfloat16
    core = lax.rem(z, 2)
    own_core = core == c
    myslot = z // 2
    sib = {"seq": 1 - c}
    upper = z >= S
    border = jnp.where(upper, S, S - 1)
    edge = jnp.where(upper, Z - 1, 0)
    near = jnp.where(upper, S - 1, 0)
    far = 1 - near
    scope = jax.named_scope

    def rcopy(src, dst, ss, rs, where):
        return pltpu.make_async_remote_copy(
            src_ref=src, dst_ref=dst, send_sem=ss, recv_sem=rs, device_id=where,
            device_id_type=pl.DeviceIdType.MESH,
        )

    def band(q, parts):
        return pl.ds(q * (rows // parts), rows // parts)

    loads = [
        pltpu.make_async_copy(src, dst, l_sem.at[i])
        for i, (src, dst) in enumerate((
            (x_hbm, x_ref), (w_hbm, w_ref), (wd_hbm, wd_ref), (wo_hbm, wo_ref), (ng_hbm, ng_ref),
            (cw_hbm, cw_ref), (cb_hbm, cb_ref), (db_hbm, db_ref), (dr_hbm, dr_ref), (sk_hbm, sk_ref),
            (ig_hbm, ig_ref)))
    ]
    for load in loads:
        load.start()
    barrier = pltpu.get_barrier_semaphore()
    for d in range(Z):
        for e in range(2):
            @pl.when(jnp.logical_not(jnp.logical_and(d == z, e == c)))
            def _():
                pl.semaphore_signal(barrier, inc=1, device_id={"dp": d, "seq": e},
                                    device_id_type=pl.DeviceIdType.MESH)
    for s in (nxt, prv):
        pl.semaphore_signal(barrier, inc=1, device_id={"section": s},
                            device_id_type=pl.DeviceIdType.MESH)

    def row0(core, chip):
        return pl.multiple_of((core * Z + chip) * KR, KR)

    lanes = d2.shape[2]
    loads[2].wait()
    for d in range(Z):
        two = jnp.concatenate(
            [wd_ref[d * hper : (d + 1) * hper, :].astype(f32),
             wd_ref[(Z + d) * hper : (Z + d + 1) * hper, :].astype(f32),
             jnp.zeros((16 - 2 * hper, KR), f32)], axis=0)
        d2[d] = jnp.concatenate([two, jnp.zeros((16, lanes - KR), f32)], axis=1).astype(bf16)
    dbuf[c * Z + z] = d2[z]
    loads[0].wait()
    loads[1].wait()
    for d in range(Z):
        w2[d, :, 0:per] = w_ref[:, d * per : (d + 1) * per]
        w2[d, :, per:VC] = w_ref[:, Z * per + d * per : Z * per + (d + 1) * per]
        w2[d, :, VC:CC] = w_ref[:, INNER : INNER + NB]

    with scope("barrier"):
        pl.semaphore_wait(barrier, 2 * Z - 1 + 2)

    def i_copy(q, way):
        where = sib if way == 0 else {"dp": z + (1 if way == 1 else -1), "seq": core}
        at = band(0, 1) if q is None else band(q, QX)
        q = q or 0
        return rcopy(x_ref.at[at], sbuf.at[myslot, c, at], i_send.at[way], s_recv.at[myslot, c, q], where)

    inner, outer = z == border, z != border
    ways = ((0, jnp.logical_not(own_core)), (1, z + 1 < Z), (2, z > 0))
    summer = jnp.logical_and(inner, own_core)
    joiner = jnp.logical_and(inner, jnp.logical_not(own_core))

    def send_x(on, inward):
        for way, there in ways[1:]:
            towards = jnp.logical_xor(upper, way == 1)
            if inward:
                there = jnp.logical_and(there, outer)
            @pl.when(jnp.logical_and(jnp.logical_and(on, there), towards if inward else jnp.logical_not(towards)))
            def _():
                for q in range(QX):
                    i_copy(q, way).start()

    def s_copy(k, h, q, up):
        at = band(0, 1) if q is None else band(q, QX)
        q = q or 0
        return rcopy(sbuf.at[k, h, at], sbuf.at[k, h, at], s_send.at[k, h], s_recv.at[k, h, q],
                     {"dp": z + (1 if up else -1)})

    def relay(k, h, q, fn):
        b = 2 * k + c
        @pl.when(jnp.logical_and(z > b, z + 1 < Z))
        def _():
            fn(s_copy(k, h, q, True))
        @pl.when(jnp.logical_and(z < b, z > 0))
        def _():
            fn(s_copy(k, h, q, False))

    def own_on(h, q, fn):
        at = band(0, 1) if q is None else band(q, QX)
        @pl.when(summer)
        def _():
            fn(rcopy(sbuf.at[near, h, at], sbuf.at[near, h, at], s_send.at[near, h],
                     s_recv.at[near, h, q or 0], {"dp": jnp.where(upper, z - 1, z + 1)}))

    def pass_on(k, h, chunks=range(QX)):
        for q in chunks:
            @pl.when(jnp.logical_not(jnp.logical_and(own_core, jnp.logical_and(k == myslot, h == c))))
            def _():
                s_copy(k, h, q, True).wait_recv()
            relay(k, h, q, lambda cp: cp.start())


    def pass_at(k, h, on, chunks=range(QX)):
        @pl.when(on)
        def _():
            pass_on(k, h, chunks)

    one, two = jnp.where(inner, far, near), jnp.where(inner, near, far)

    def w_copies(d, frm):
        at = pl.ds(row0(c, frm), KR)
        g = c * Z + frm
        return (rcopy(w2.at[d], wbuf.at[at], w_send, w_recv.at[frm], {"dp": d}),
                rcopy(d2.at[d], dbuf.at[g], d_send, d_recv.at[frm], {"dp": d}))

    def f_copies(d, core):
        at = pl.ds(row0(core, d), KR)
        g = core * Z + d
        return (rcopy(wbuf.at[at], wbuf.at[at], f_send, f_recv, sib),
                rcopy(dbuf.at[g], dbuf.at[g], g_send, g_recv, sib))

    def forwards():
        half = pl.ds(0, Z * KR)
        return (rcopy(wbuf.at[half], wbuf.at[half], f_send, f_recv, sib),
                rcopy(dbuf.at[pl.ds(0, Z)], dbuf.at[pl.ds(0, Z)], g_send, g_recv, sib))

    def send_w(d, on):
        @pl.when(on)
        def _():
            for cp in w_copies(d, z):
                cp.start()

    @pl.when(own_core)
    def _():
        sbuf[myslot, c] = x_ref[...]

    with scope("early"):
        @pl.when(ways[0][1])
        def _():
            for q in range(QX):
                i_copy(q, 0).start()
        send_x(c == 0, True)
        send_x(c == 0, False)
        @pl.when(c == 0)
        def _():
            for q in range(QX):
                own_on(0, q, lambda cp: cp.start())
        send_w(jnp.where(upper, 0, Z - 1), inner)
        send_w(edge, inner)
        for step in (3, 1, 2):
            send_w(jnp.where(upper, z - step, z + step), outer)
        own_fwd = (
            rcopy(w2.at[z], wbuf.at[pl.ds(row0(c, z), KR)], f_send, f_recv, sib),
            rcopy(d2.at[z], dbuf.at[c * Z + z], g_send, g_recv, sib),
        )
        for cp in own_fwd:
            cp.start()
        wbuf[pl.ds(row0(c, z), KR), :] = w2[z]
        pass_at(near, 0, inner)
        @pl.when(c == 1)
        def _():
            for q in range(QX):
                own_on(0, q, lambda cp: cp.start())
        send_w(jnp.where(upper, S - 1, S), inner)
        send_x(jnp.logical_and(c == 1, outer), True)

    loads[3].wait()
    at_wo = pl.ds(pl.multiple_of(c * per, per), per)
    wo_copy = rcopy(wo_ref, wobuf.at[at_wo], o_send, o_recv, sib)
    wo_copy.start()
    wobuf[at_wo, :] = wo_ref[...]
    for load in loads[4:]:
        load.wait()

    def pick(ref, width, tail):
        wide = Z * width
        got = None
        for d in range(Z):
            part = jnp.concatenate(
                [ref[:, d * width : (d + 1) * width],
                 ref[:, wide + d * width : wide + (d + 1) * width]], axis=1)
            part = jnp.where(z == d, part, 0.0)
            got = part if got is None else got + part
        return jnp.concatenate([got, tail], axis=1) if tail is not None else got

    gain_in = ng_ref[...]
    hi = lax.Precision.HIGHEST
    taps = pick(cw_ref, per, cw_ref[:, INNER : INNER + NB])
    tbias = pick(cb_ref, per, cb_ref[:, INNER : INNER + NB])
    hz = jnp.zeros((1, 128 - 2 * hper), f32)
    heads = jnp.concatenate(
        [pick(db_ref, hper, hz), pick(dr_ref, hper, hz), pick(sk_ref, hper, hz),
         jnp.zeros((5, 128), f32)], axis=0)
    heads_t = heads.T[0:16]
    dtb, rate = heads_t[:, 0:1], heads_t[:, 1:2]
    gain_out = pick(ig_ref, per, None)
    spread = (lax.broadcasted_iota(jnp.int32, (16, VC), 1) // HEAD_DIM
              == lax.broadcasted_iota(jnp.int32, (16, VC), 0)).astype(f32)

    def widen(m):
        return jnp.dot(m, spread, precision=hi, preferred_element_type=f32)

    skip_wide = widen(heads[:, 0:16])[2:3]
    ii = lax.broadcasted_iota(jnp.int32, (BLOCK, BLOCK), 0)
    jj = lax.broadcasted_iota(jnp.int32, (BLOCK, BLOCK), 1)
    causal = ii >= jj
    triu = (ii <= jj).astype(f32)
    low_lane = lax.broadcasted_iota(jnp.int32, (BLOCK, 128), 1) < HEAD_DIM
    margin = CONV - 1

    def norm_in(k, h):
        v = sbuf[k, h].astype(f32)
        ms = jnp.mean(v * v, axis=-1, keepdims=True)
        nbuf[k, h] = (v * lax.rsqrt(ms + epsilon) * gain_in).astype(bf16)

    def unit(k, h, hook=None):
        nb = nbuf[k, h]
        if h == 0:
            cbuf[0:8, :] = jnp.zeros((8, CC), f32)
        else:
            cbuf[0:8, :] = tails[k]
        cbuf[8 : 8 + rows, :] = jnp.dot(nb, wbuf[...], preferred_element_type=f32).astype(bf16).astype(f32)
        if h == 0:
            tails[k] = cbuf[rows : rows + 8, :]
        acc = jnp.broadcast_to(tbias, (rows, CC))
        for t in range(CONV):
            acc = acc + taps[t : t + 1, :] * cbuf[8 - margin + t : 8 - margin + t + rows, :]
        vbuf[...] = (acc / (1.0 + jnp.exp(-acc))).astype(bf16)
        if hook is not None:
            hook()
        raw = lax.dot_general(w_steps, nb, (((1,), (1,)), ((), ())), preferred_element_type=f32) + dtb
        dt_t = jnp.maximum(raw, 0.0) + jnp.log1p(jnp.exp(-jnp.abs(raw)))
        cum_t = jnp.dot(-dt_t * rate, triu, precision=hi, preferred_element_type=f32)
        tail_t = jnp.exp(cum_t[:, BLOCK - 1 : BLOCK] - cum_t) * dt_t
        cols = jnp.concatenate([cum_t, tail_t, jnp.exp(cum_t), jnp.zeros((80, BLOCK), f32)], axis=0).T
        cum = cols[:, 0:16]
        bm = vbuf[:, VC : VC + STATE]
        cm = vbuf[:, VC + STATE : CC]
        scores = lax.dot_general(cm, bm, (((1,), (1,)), ((), ())), preferred_element_type=f32)
        scores = jnp.where(causal, scores, 0.0)
        vals = vbuf[:, 0:VC].astype(f32)
        part = skip_wide * vals
        if h > 0:
            grow = widen(cols[:, 32:48])
            part = part + grow * jnp.dot(cm.astype(f32), state[k], precision=hi,
                                         preferred_element_type=f32)
        for p in range(VC // 128):
            mix = []
            for q in range(2):
                hd = 2 * p + q
                lag = cum[:, hd : hd + 1] - cum_t[hd : hd + 1, :]
                m = scores * jnp.exp(jnp.minimum(lag, 0.0)) * dt_t[hd : hd + 1, :]
                mix.append(m.astype(bf16))
            vp = vals[:, p * 128 : (p + 1) * 128]
            two = jnp.concatenate([jnp.where(low_lane, vp, 0.0), jnp.where(low_lane, 0.0, vp)],
                                  axis=0).astype(bf16)
            got = jnp.dot(jnp.concatenate(mix, axis=1), two, preferred_element_type=f32)
            ybuf[:, p * 128 : (p + 1) * 128] = got + part[:, p * 128 : (p + 1) * 128]
        y = ybuf[...]
        pbuf[k, h] = jnp.dot((y * gain_out).astype(bf16), wobuf[...], preferred_element_type=f32).astype(bf16)
        stbuf[k, h] = lax.dot_general(jnp.ones((8, VC), f32), y * y, (((1,), (1,)), ((), ())),
                                      precision=hi, preferred_element_type=f32)
        if h == 0:
            scaled = (vals * widen(cols[:, 16:32])).astype(bf16)
            state[k] = lax.dot_general(bm, scaled, (((0,), (0,)), ((), ())), preferred_element_type=f32)

    def place(b, h):
        return {"dp": b, "seq": h}

    def here(h):
        return jnp.logical_and(own_core, h == c)

    def p_copies(h, whole=False):
        slot = lax.rem(z, S)
        where = place(2 * near + c, h)
        parts = 1 if whole else QP
        return (rcopy(stbuf.at[near, h], rstat.at[slot], t_send.at[near, h], t_recv.at[slot], where),
                *(rcopy(pbuf.at[near, h, band(q, parts)], rpart.at[slot, band(q, parts)], p_send.at[h],
                        p_recv.at[slot, q], where) for q in range(parts)))

    def x_copies(h, q):
        at, q = (band(0, 1), 0) if q is None else (band(q, QP), q)
        big = rcopy(pbuf.at[far, h, at], xpart.at[h, at], q_send.at[h], x_recv.at[h, q], {"dp": border})
        if q > 0:
            return (big,)
        return (rcopy(stbuf.at[far, h], xstat.at[h], t_send.at[far, h], y_recv.at[h], {"dp": border}), big)

    def b_copies(h, q, join):
        at, q = (band(0, 1), 0) if q is None else (band(q, QP), q)
        if join:
            where = {"dp": Z - 1 - z}
            big, small = (kpart.at[h, at], k_recv.at[h, q]), (kstat.at[h], kt_recv.at[h])
        else:
            where = place(2 * far + c, h)
            big, small = (rpart.at[S, at], p_recv.at[S, q]), (rstat.at[S], t_recv.at[S])
        big = rcopy(bpart.at[h, at], big[0], b_send.at[h], big[1], where)
        if q > 0:
            return (big,)
        return (rcopy(bstat.at[h], small[0], c_send.at[h], small[1], where), big)

    def j_copies(h, q):
        where = place(edge, h)
        at, q = (band(0, 1), 0) if q is None else (band(q, QP), q)
        big = rcopy(jpart.at[h, at], rpart.at[S, at], j_send.at[h], p_recv.at[S, q], where)
        if q > 0:
            return (big,)
        return (rcopy(jstat.at[h], rstat.at[S], jt_send.at[h], t_recv.at[S], where), big)

    def join_near(h, chunks=range(QP)):
        @pl.when(joiner)
        def _():
            for q in chunks:
                at = band(q, QP)
                for cp in b_copies(h, q, True):
                    cp.wait_recv()
                jpart[h, at] = (pbuf[near, h, at].astype(f32) + kpart[h, at].astype(f32)).astype(bf16)
                if q == 0:
                    jstat[h] = stbuf[near, h] + kstat[h]
                for cp in j_copies(h, q):
                    cp.start()

    def send_far(h):
        @pl.when(outer)
        def _():
            for q in range(QP):
                for cp in x_copies(h, q):
                    cp.start()

    def send_near(h, now):
        @pl.when(jnp.logical_and(now, here(h)))
        def _():
            rpart[lax.rem(z, S)] = pbuf[near, h]
            rstat[lax.rem(z, S)] = stbuf[near, h]

        @pl.when(jnp.logical_and(jnp.logical_and(now, jnp.logical_not(joiner)), jnp.logical_not(here(h))))
        def _():
            for cp in p_copies(h):
                cp.start()

    def sum_far(h, chunks=range(QP), on=True):
        @pl.when(jnp.logical_and(inner, on))
        def _():
            for q in chunks:
                at = band(q, QP)
                for cp in x_copies(h, q):
                    cp.wait_recv()
                bpart[h, at] = (pbuf[far, h, at].astype(f32) + xpart[h, at].astype(f32)).astype(bf16)
                if q == 0:
                    bstat[h] = stbuf[far, h] + xstat[h]
                for on, join in ((own_core, True), (jnp.logical_not(own_core), False)):
                    @pl.when(on)
                    def _():
                        for cp in b_copies(h, q, join):
                            cp.start()

    with scope("passf0i"):
        pass_at(far, 0, inner)
    with scope('passn1i'):
        pass_at(near, 1, joiner)
    for step in range(1, Z):
        for d in (z + step, z - step):
            @pl.when(jnp.logical_and(d >= 0, d < Z))
            def _():
                with scope(f"wrecv{step}"):
                    for cp in w_copies(z, d):
                        cp.wait_recv()
                for cp in f_copies(d, c):
                    cp.start()
    with scope("fwait"):
        for cp in forwards():
            cp.wait_recv()
        wo_copy.wait_recv()
    w_steps = jnp.concatenate([dbuf[g][:, 0:KR].astype(f32) for g in range(2 * Z)], axis=1).astype(bf16)

    def r_copies(j, q):
        at = band(q, QP)
        big = rcopy(pbuf.at[0, 0, at], rpart.at[j, at], p_send.at[0], p_recv.at[j, q], sib)
        if q > 0:
            return (big,)
        return (rcopy(stbuf.at[0, 0], rstat.at[j], t_send.at[0, 0], t_recv.at[j], sib), big)

    def e_copy(q, parts=QP):
        at = band(q, parts)
        return rcopy(obuf.at[at], out_ref.at[at], e_send, e_recv, {"section": nxt})

    def finish():
        scale = None
        for q in range(QP):
            at = band(q, QP)
            with scope(f"rwait{q}"):
                for j in range(S + 1):
                    own = lax.rem(z, S) == j
                    take = jnp.logical_or(jnp.logical_and(own, jnp.logical_not(own_core)),
                                          jnp.logical_and(inner, jnp.logical_not(own))) if j < S else True
                    @pl.when(take)
                    def _():
                        for cp in r_copies(j, q):
                            cp.wait_recv()
            if q == 0:
                stat = rstat[S]
                for j in range(S):
                    stat = stat + jnp.where(jnp.logical_or(inner, lax.rem(z, S) == j), rstat[j], 0.0)
                scale = lax.rsqrt(stat * (1.0 / INNER) + epsilon).T[:, 0:1]
            total = rpart[S, at].astype(f32)
            for j in range(S):
                part = rpart[j, at].astype(f32)
                total = total + jnp.where(jnp.logical_or(inner, lax.rem(z, S) == j), part, 0.0)
            size = rows // QP
            obuf[at, :] = (x_ref[at].astype(f32) + total * scale[q * size : (q + 1) * size]).astype(bf16)
            e_copy(q).start()

    with scope('own1'):
        pass_at(near, 1, summer)
        for q in range(QX):
            own_on(1, q, lambda cp: cp.start())

    with scope("passf1h"):
        pass_at(far, 1, summer)
    with scope("passn0"):
        pass_at(near, 0, outer)
    with scope("unit0"):
        norm_in(one, 0)
        unit(one, 0, lambda: pass_at(far, 1, joiner, (0,)))
    with scope("passf1i"):
        pass_at(far, 1, joiner, (1,))
    send_x(jnp.logical_and(c == 1, inner), False)
    with scope("passf0"):
        pass_at(far, 0, outer)
    with scope("unit1"):
        norm_in(two, 0)
        unit(two, 0, lambda: pass_at(far, 1, joiner, (2,)))
    send_far(0)
    send_near(0, outer)
    with scope("passf1j"):
        pass_at(far, 1, joiner, (3,))
    with scope("sumf0"):
        sum_far(0)
    with scope("passf1"):
        pass_at(far, 1, outer)
    with scope("unit2"):
        norm_in(far, 1)
        unit(far, 1)
    send_far(1)
    with scope("sums1"):
        sum_far(1, on=summer)
    send_near(0, inner)
    with scope("passn1"):
        pass_at(near, 1, outer)
    with scope("unit3"):
        norm_in(near, 1)
        unit(near, 1)
    send_near(1, inner)
    send_near(1, outer)
    with scope("join0"):
        join_near(0)
    with scope("fin0"):
        @pl.when(c == 0)
        def _():
            finish()
    with scope("join1"):
        join_near(1)
    with scope("sumf1"):
        sum_far(1, on=joiner)
    with scope("fin1"):
        @pl.when(c == 1)
        def _():
            finish()
    with scope("sends"):
        for way, on in ways:
            on = on if way == 0 else jnp.logical_and(on, jnp.logical_or(outer, jnp.logical_xor(upper, way == 2)))
            @pl.when(on)
            def _():
                i_copy(None, way).wait_send()
        wo_copy.wait_send()
        for cp in forwards():
            cp.wait_send()
        others = pl.ds(0, Z - 1)
        rcopy(w2.at[others], w2.at[others], w_send, w_recv.at[0], sib).wait_send()
        rcopy(d2.at[others], d2.at[others], d_send, d_recv.at[0], sib).wait_send()
        for h in range(2):
            for k in range(S):
                relay(k, h, None, lambda cp: cp.wait_send())
            own_on(h, None, lambda cp: cp.wait_send())
            @pl.when(outer)
            def _():
                for cp in x_copies(h, None):
                    cp.wait_send()
            @pl.when(inner)
            def _():
                for cp in b_copies(h, None, True):
                    cp.wait_send()
            @pl.when(joiner)
            def _():
                for cp in j_copies(h, None):
                    cp.wait_send()
            @pl.when(jnp.logical_not(jnp.logical_or(joiner, here(h))))
            def _():
                for cp in p_copies(h, True):
                    cp.wait_send()
    with scope("last"):
        e_copy(0, 1).wait()


def fused(
    stream, norm_gain, w_xbc, w_dt, conv_weight, conv_bias, dt_bias, decay_rate, skip_weight,
    inner_gain, w_out,
):
    Z = lax.axis_size("dp")
    rows, D = stream.shape[2:]
    if rows != BLOCK:
        return shards(stream, norm_gain, w_xbc, w_dt, conv_weight, conv_bias, dt_bias, decay_rate,
                      skip_weight, inner_gain, w_out)
    KR = w_xbc.shape[1]
    VC = INNER // Z
    CC = VC + 2 * STATE
    S = Z // 2
    lanes = -(-KR // 128) * 128
    bf16, f32 = jnp.bfloat16, jnp.float32
    dma, V = pltpu.SemaphoreType.DMA, pltpu.VMEM
    far, held = pl.BlockSpec(memory_space=pltpu.HBM), pl.BlockSpec(memory_space=pltpu.VMEM)
    out = pl.pallas_call(
        functools.partial(section_kernel, Z),
        out_shape=jax.ShapeDtypeStruct((rows, D), bf16),
        in_specs=[far] * 11,
        out_specs=pl.BlockSpec(memory_space=pl.ANY),
        scratch_shapes=[
            V((rows, D), bf16), V(norm_gain.shape, f32), V(w_xbc.shape[1:], bf16),
            V((HEADS, KR), bf16), V(conv_weight.shape[1:], f32), V(conv_bias.shape, f32),
            V(dt_bias.shape, f32), V(dt_bias.shape, f32), V(dt_bias.shape, f32),
            V(inner_gain.shape, f32), V(w_out.shape[1:], bf16),
            V((Z, KR, CC), bf16), V((2 * Z * KR, CC), bf16),
            V((Z, 16, lanes), bf16), V((2 * Z, 16, lanes), bf16),
            V((VC, D), bf16),
            V((S, 2, rows, D), bf16), V((S, 2, rows, D), bf16),
            V((8 + rows, CC), f32), V((S, 8, CC), f32), V((rows, CC), bf16), V((rows, VC), f32),
            V((S, STATE, VC), f32),
            V((S, 2, rows, D), bf16), V((S, 2, 8, rows), f32),
            V((2, rows, D), bf16), V((2, 8, rows), f32),
            V((2, rows, D), bf16), V((2, 8, rows), f32),
            V((2, rows, D), bf16), V((2, 8, rows), f32),
            V((2, rows, D), bf16), V((2, 8, rows), f32),
            V((S + 1, rows, D), bf16), V((S + 1, 8, rows), f32),
            V((rows, D), bf16),
            dma((11,)), dma, dma((Z,)), dma, dma((Z,)), dma, dma, dma, dma, dma, dma,
            dma((3,)), dma((S, 2)), dma((S, 2, QX)), dma, dma, dma((2,)), dma((S + 1, QP)),
            dma((S, 2)), dma((S + 1,)),
            dma((2,)), dma((2, QP)), dma((2,)), dma((2,)), dma((2,)), dma((2, QP)), dma((2,)),
            dma((2,)), dma((2,)),
        ],
        compiler_params=pltpu.CompilerParams(
            collective_id=0, has_side_effects=True, vmem_limit_bytes=50 * 1024 * 1024
        ),
    )(
        *(pltpu.with_memory_space_constraint(a, pltpu.HBM) for a in (
            stream[0, 0], norm_gain, w_xbc[0], jnp.swapaxes(w_dt, 1, 2)[0], conv_weight[0], conv_bias,
            dt_bias, decay_rate, skip_weight, inner_gain, w_out[0]))
    )
    return out[None, None]


def solution(mesh):
    placed = (
        P("section", "dp", "seq", None),
        P("section", None),
        P("section", ("seq", "dp"), None),
        P("section", ("seq", "dp"), None),
        P("section", None, None),
        P("section", None),
        P("section", None),
        P("section", None),
        P("section", None),
        P("section", None),
        P("section", ("seq", "dp"), None),
    )
    size = mesh.shape
    chips = size["dp"]
    whole_heads = HEADS % (2 * chips) == 0 and (INNER // chips) % 128 == 0
    body = fused if size["seq"] == 2 and chips == 4 and whole_heads and size["section"] > 1 else shards
    return jax.shard_map(
        body,
        mesh=mesh,
        in_specs=placed,
        out_specs=P("section", "dp", "seq", None),
        check_vma=False,
    )
```

```python
import functools

import jax
import jax.numpy as jnp
from jax import lax
from jax.experimental import pallas as pl
from jax.experimental.pallas import tpu as pltpu
from jax.sharding import PartitionSpec as P

HEADS = 40
HEAD_DIM = 64
STATE = 64
CONV = 4
BLOCK = 128
INNER = 2560


epsilon = 1e-05
QX = 4
QP = 4


def prefix(x, axis, combine, identity):
    devices, position = (lax.axis_size(axis), lax.axis_index(axis))
    everything = jax.tree.map(
        lambda part, kind: lax.all_gather(part.astype(kind), axis),
        x,
        jax.tree.map(lambda a: jnp.bfloat16 if a.dtype == jnp.float32 else a.dtype, x),
    )
    start = jax.tree.map(
        lambda part, zero: jnp.broadcast_to(jnp.asarray(zero, part.dtype), part.shape), x, identity
    )

    def hop(k, before):
        reached = k < position
        new = combine(
            before, jax.tree.map(lambda part, own: part[k].astype(own.dtype), everything, x)
        )
        return jax.tree.map(lambda a, b: jnp.where(reached, a, b), new, before)

    return lax.fori_loop(0, devices, hop, start)


def from_behind(x, axis, by):
    devices = lax.axis_size(axis)
    pairs = [(i, i + by) for i in range(devices) if 0 <= i + by < devices]
    return lax.ppermute(x, axis, pairs)


def passed_along(x, axis, by):
    devices = lax.axis_size(axis)
    return lax.ppermute(x, axis, [(i, (i + by) % devices) for i in range(devices)])


def rms_scale(values, scale_gain):
    mean_square = jnp.mean(values * values, axis=-1, keepdims=True)
    return values * lax.rsqrt(mean_square + epsilon) * scale_gain


def block_terms(values, b_rows, c_rows, dt_rows, head_rates):
    block_len = dt_rows.shape[0]
    cum_decay = jnp.cumsum(-dt_rows * head_rates[None, :], axis=0)
    scores = jnp.dot(c_rows, b_rows.T, preferred_element_type=jnp.float32)
    lag_decay = cum_decay.T[:, :, None] - cum_decay.T[:, None, :]
    causal = jnp.arange(block_len)[:, None] >= jnp.arange(block_len)[None, :]
    weights = jnp.where(causal[None], jnp.exp(jnp.minimum(lag_decay, 0.0)), 0.0)
    mixing = (scores[None] * weights * dt_rows.T[:, None, :]).astype(jnp.bfloat16)
    intra_out = jnp.einsum("hij,jhp->ihp", mixing, values, preferred_element_type=jnp.float32)
    tail_weight = jnp.exp(cum_decay[-1][None, :] - cum_decay) * dt_rows
    scaled = (values.astype(jnp.float32) * tail_weight[:, :, None]).astype(jnp.bfloat16)
    summary = jnp.einsum("jhp,jn->hpn", scaled, b_rows, preferred_element_type=jnp.float32)
    return (intra_out, summary, jnp.exp(cum_decay[-1]), jnp.exp(cum_decay))


def state_output(c_rows, growth, carried):
    readout = jnp.einsum(
        "in,hpn->ihp", c_rows.astype(jnp.float32), carried, precision=lax.Precision.HIGHEST
    )
    return growth[:, :, None] * readout


def combine_states(earlier, latest):
    decay_a, state_a = earlier
    decay_b, state_b = latest
    return (decay_a * decay_b, decay_b[:, None] * state_a + state_b)


def chain_states(summary):
    identity = (jnp.ones_like(summary[0]), jnp.zeros_like(summary[1]))
    return prefix(summary, "seq", combine_states, identity)


def project_rows(normed_rows, xbc_part, dt_part):
    return (
        jnp.dot(
            normed_rows,
            lax.all_gather(xbc_part, ("seq", "dp"), axis=0, tiled=True),
            preferred_element_type=jnp.float32,
        ),
        jnp.dot(
            normed_rows,
            lax.all_gather(dt_part, ("seq", "dp"), axis=0, tiled=True),
            preferred_element_type=jnp.float32,
        ),
    )


def shards(
    stream,
    norm_gain,
    w_xbc,
    w_dt,
    conv_weight,
    conv_bias,
    dt_bias,
    decay_rate,
    skip_weight,
    inner_gain,
    w_out,
):
    rows_in = stream[0, 0]
    length_dev = rows_in.shape[0]
    margin = CONV - 1
    row_gain = norm_gain[0]
    normed = rms_scale(rows_in.astype(jnp.float32), row_gain).astype(jnp.bfloat16)
    projected, dt_raw = project_rows(normed, w_xbc[0], w_dt[0])
    xbc_raw = projected.astype(jnp.bfloat16)
    prev_proj = from_behind(xbc_raw[length_dev - margin :], "seq", 1)
    padded = jnp.concatenate([prev_proj, xbc_raw], axis=0)
    conv_sum = jnp.broadcast_to(conv_bias[0][None, :], (length_dev, padded.shape[1]))
    for tap_index in range(CONV):
        conv_sum = conv_sum + conv_weight[0, tap_index][None, :] * padded[
            tap_index : tap_index + length_dev
        ].astype(jnp.float32)
    mixed_rows = jax.nn.silu(conv_sum).astype(jnp.bfloat16)
    blocks = length_dev // BLOCK
    values = mixed_rows[:, :INNER].reshape(blocks, BLOCK, HEADS, HEAD_DIM)
    b_rows = mixed_rows[:, INNER : INNER + STATE].reshape(blocks, BLOCK, STATE)
    c_rows = mixed_rows[:, INNER + STATE :].reshape(blocks, BLOCK, STATE)
    dt_rows = jax.nn.softplus(dt_raw + dt_bias[0][None, :]).reshape(blocks, BLOCK, HEADS)
    intra_out, summary, totals, growth = jax.vmap(block_terms, in_axes=(0, 0, 0, 0, None))(
        values, b_rows, c_rows, dt_rows, decay_rate[0]
    )

    def local_step(running, inputs):
        carried, decay_before = running
        block_total, block_summary = inputs
        return (
            (block_total[:, None, None] * carried + block_summary, decay_before * block_total),
            (carried, decay_before),
        )

    start_state = (
        jnp.zeros((HEADS, HEAD_DIM, STATE), jnp.float32),
        jnp.ones((HEADS,), jnp.float32),
    )
    (local_state, local_decay), (enter_local, decay_before) = lax.scan(
        local_step, start_state, (totals, summary)
    )
    state_terms = jax.vmap(state_output)
    early_terms = state_terms(c_rows, growth, enter_local)
    incoming_decay, incoming_flat = chain_states(
        (local_decay, local_state.reshape(HEADS, HEAD_DIM * STATE))
    )
    arriving = incoming_flat.reshape(HEADS, HEAD_DIM, STATE)
    late_terms = state_terms(c_rows, growth, decay_before[:, :, None, None] * arriving[None])
    state_part = early_terms + late_terms
    mixed_out = (
        intra_out + state_part + skip_weight[0][None, None, :, None] * values.astype(jnp.float32)
    )
    normed_out = rms_scale(mixed_out.reshape(length_dev, INNER), inner_gain[0]).astype(jnp.bfloat16)
    branch_out = jnp.dot(
        normed_out,
        lax.all_gather(w_out[0], ("seq", "dp"), axis=0, tiled=True),
        preferred_element_type=jnp.float32,
    )
    next_rows = (rows_in.astype(jnp.float32) + branch_out).astype(jnp.bfloat16)
    shifted = passed_along(next_rows, "section", 1)
    return shifted[None, None]

def section_kernel(
    Z, x_hbm, ng_hbm, w_hbm, wd_hbm, cw_hbm, cb_hbm, db_hbm, dr_hbm, sk_hbm, ig_hbm, wo_hbm,
    out_ref,
    x_ref, ng_ref, w_ref, wd_ref, cw_ref, cb_ref, db_ref, dr_ref, sk_ref, ig_ref, wo_ref, w2,
    wbuf, d2, dbuf, wobuf, sbuf, nbuf, cbuf, tails, vbuf, ybuf, state,
    pbuf, stbuf, xpart, xstat, bpart, bstat, kpart, kstat, jpart, jstat, rpart, rstat, obuf,
    l_sem, w_send, w_recv, d_send, d_recv, f_send, f_recv, g_send, g_recv, o_send, o_recv,
    i_send, s_send, s_recv, e_send, e_recv, p_send, p_recv, t_send, t_recv,
    q_send, x_recv, y_recv, b_send, c_send, k_recv, kt_recv, j_send, jt_send,
):
    z = lax.axis_index("dp")
    c = lax.axis_index("seq")
    sec = lax.axis_index("section")
    NS = lax.axis_size("section")
    nxt = lax.rem(sec + 1, NS)
    prv = lax.rem(sec + NS - 1, NS)
    S = Z // 2
    rows, D = x_ref.shape
    KR = w_ref.shape[0]
    per = INNER // (2 * Z)
    hper = HEADS // (2 * Z)
    VC = 2 * per
    NB = 2 * STATE
    CC = VC + NB
    f32, bf16 = jnp.float32, jnp.bfloat16
    core = lax.rem(z, 2)
    own_core = core == c
    myslot = z // 2
    sib = {"seq": 1 - c}
    upper = z >= S
    border = jnp.where(upper, S, S - 1)
    edge = jnp.where(upper, Z - 1, 0)
    near = jnp.where(upper, S - 1, 0)
    far = 1 - near
    scope = jax.named_scope

    def rcopy(src, dst, ss, rs, where):
        return pltpu.make_async_remote_copy(
            src_ref=src, dst_ref=dst, send_sem=ss, recv_sem=rs, device_id=where,
            device_id_type=pl.DeviceIdType.MESH,
        )

    def band(q, parts):
        return pl.ds(q * (rows // parts), rows // parts)

    loads = [
        pltpu.make_async_copy(src, dst, l_sem.at[i])
        for i, (src, dst) in enumerate((
            (x_hbm, x_ref), (w_hbm, w_ref), (wd_hbm, wd_ref), (wo_hbm, wo_ref), (ng_hbm, ng_ref),
            (cw_hbm, cw_ref), (cb_hbm, cb_ref), (db_hbm, db_ref), (dr_hbm, dr_ref), (sk_hbm, sk_ref),
            (ig_hbm, ig_ref)))
    ]
    for load in loads:
        load.start()
    barrier = pltpu.get_barrier_semaphore()
    for d in range(Z):
        for e in range(2):
            @pl.when(jnp.logical_not(jnp.logical_and(d == z, e == c)))
            def _():
                pl.semaphore_signal(barrier, inc=1, device_id={"dp": d, "seq": e},
                                    device_id_type=pl.DeviceIdType.MESH)
    for s in (nxt, prv):
        pl.semaphore_signal(barrier, inc=1, device_id={"section": s},
                            device_id_type=pl.DeviceIdType.MESH)

    def row0(core, chip):
        return pl.multiple_of((core * Z + chip) * KR, KR)

    lanes = d2.shape[2]
    loads[2].wait()
    for d in range(Z):
        two = jnp.concatenate(
            [wd_ref[d * hper : (d + 1) * hper, :].astype(f32),
             wd_ref[(Z + d) * hper : (Z + d + 1) * hper, :].astype(f32),
             jnp.zeros((16 - 2 * hper, KR), f32)], axis=0)
        d2[d] = jnp.concatenate([two, jnp.zeros((16, lanes - KR), f32)], axis=1).astype(bf16)
    dbuf[c * Z + z] = d2[z]
    loads[0].wait()
    loads[1].wait()
    for d in range(Z):
        w2[d, :, 0:per] = w_ref[:, d * per : (d + 1) * per]
        w2[d, :, per:VC] = w_ref[:, Z * per + d * per : Z * per + (d + 1) * per]
        w2[d, :, VC:CC] = w_ref[:, INNER : INNER + NB]

    with scope("barrier"):
        pl.semaphore_wait(barrier, 2 * Z - 1 + 2)

    def i_copy(q, way):
        where = sib if way == 0 else {"dp": z + (1 if way == 1 else -1), "seq": core}
        at = band(0, 1) if q is None else band(q, QX)
        q = q or 0
        return rcopy(x_ref.at[at], sbuf.at[myslot, c, at], i_send.at[way], s_recv.at[myslot, c, q], where)

    inner, outer = z == border, z != border
    ways = ((0, jnp.logical_not(own_core)), (1, z + 1 < Z), (2, z > 0))
    summer = jnp.logical_and(inner, own_core)
    joiner = jnp.logical_and(inner, jnp.logical_not(own_core))

    def send_x(on, inward):
        for way, there in ways[1:]:
            towards = jnp.logical_xor(upper, way == 1)
            if inward:
                there = jnp.logical_and(there, outer)
            @pl.when(jnp.logical_and(jnp.logical_and(on, there), towards if inward else jnp.logical_not(towards)))
            def _():
                for q in range(QX):
                    i_copy(q, way).start()

    def s_copy(k, h, q, up):
        at = band(0, 1) if q is None else band(q, QX)
        q = q or 0
        return rcopy(sbuf.at[k, h, at], sbuf.at[k, h, at], s_send.at[k, h], s_recv.at[k, h, q],
                     {"dp": z + (1 if up else -1)})

    def relay(k, h, q, fn):
        b = 2 * k + c
        @pl.when(jnp.logical_and(z > b, z + 1 < Z))
        def _():
            fn(s_copy(k, h, q, True))
        @pl.when(jnp.logical_and(z < b, z > 0))
        def _():
            fn(s_copy(k, h, q, False))

    def own_on(h, q, fn):
        at = band(0, 1) if q is None else band(q, QX)
        @pl.when(summer)
        def _():
            fn(rcopy(sbuf.at[near, h, at], sbuf.at[near, h, at], s_send.at[near, h],
                     s_recv.at[near, h, q or 0], {"dp": jnp.where(upper, z - 1, z + 1)}))

    def pass_on(k, h, chunks=range(QX)):
        for q in chunks:
            @pl.when(jnp.logical_not(jnp.logical_and(own_core, jnp.logical_and(k == myslot, h == c))))
            def _():
                s_copy(k, h, q, True).wait_recv()
            relay(k, h, q, lambda cp: cp.start())


    def pass_at(k, h, on, chunks=range(QX)):
        @pl.when(on)
        def _():
            pass_on(k, h, chunks)

    one, two = jnp.where(inner, far, near), jnp.where(inner, near, far)

    def w_copies(d, frm):
        at = pl.ds(row0(c, frm), KR)
        g = c * Z + frm
        return (rcopy(w2.at[d], wbuf.at[at], w_send, w_recv.at[frm], {"dp": d}),
                rcopy(d2.at[d], dbuf.at[g], d_send, d_recv.at[frm], {"dp": d}))

    def f_copies(d, core):
        at = pl.ds(row0(core, d), KR)
        g = core * Z + d
        return (rcopy(wbuf.at[at], wbuf.at[at], f_send, f_recv, sib),
                rcopy(dbuf.at[g], dbuf.at[g], g_send, g_recv, sib))

    def forwards():
        half = pl.ds(0, Z * KR)
        return (rcopy(wbuf.at[half], wbuf.at[half], f_send, f_recv, sib),
                rcopy(dbuf.at[pl.ds(0, Z)], dbuf.at[pl.ds(0, Z)], g_send, g_recv, sib))

    def send_w(d, on):
        @pl.when(on)
        def _():
            for cp in w_copies(d, z):
                cp.start()

    @pl.when(own_core)
    def _():
        sbuf[myslot, c] = x_ref[...]

    with scope("early"):
        @pl.when(ways[0][1])
        def _():
            for q in range(QX):
                i_copy(q, 0).start()
        send_x(c == 0, True)
        send_x(c == 0, False)
        @pl.when(c == 0)
        def _():
            for q in range(QX):
                own_on(0, q, lambda cp: cp.start())
        send_w(jnp.where(upper, 0, Z - 1), inner)
        send_w(edge, inner)
        for step in (3, 1, 2):
            send_w(jnp.where(upper, z - step, z + step), outer)
        own_fwd = (
            rcopy(w2.at[z], wbuf.at[pl.ds(row0(c, z), KR)], f_send, f_recv, sib),
            rcopy(d2.at[z], dbuf.at[c * Z + z], g_send, g_recv, sib),
        )
        for cp in own_fwd:
            cp.start()
        wbuf[pl.ds(row0(c, z), KR), :] = w2[z]
        pass_at(near, 0, inner)
        @pl.when(c == 1)
        def _():
            for q in range(QX):
                own_on(0, q, lambda cp: cp.start())
        send_w(jnp.where(upper, S - 1, S), inner)
        send_x(jnp.logical_and(c == 1, outer), True)

    loads[3].wait()
    at_wo = pl.ds(pl.multiple_of(c * per, per), per)
    wo_copy = rcopy(wo_ref, wobuf.at[at_wo], o_send, o_recv, sib)
    wo_copy.start()
    wobuf[at_wo, :] = wo_ref[...]
    for load in loads[4:]:
        load.wait()

    def pick(ref, width, tail):
        wide = Z * width
        got = None
        for d in range(Z):
            part = jnp.concatenate(
                [ref[:, d * width : (d + 1) * width],
                 ref[:, wide + d * width : wide + (d + 1) * width]], axis=1)
            part = jnp.where(z == d, part, 0.0)
            got = part if got is None else got + part
        return jnp.concatenate([got, tail], axis=1) if tail is not None else got

    gain_in = ng_ref[...]
    taps = pick(cw_ref, per, cw_ref[:, INNER : INNER + NB])
    tbias = pick(cb_ref, per, cb_ref[:, INNER : INNER + NB])
    hz = jnp.zeros((1, 128 - 2 * hper), f32)
    heads = jnp.concatenate(
        [pick(db_ref, hper, hz), pick(dr_ref, hper, hz), pick(sk_ref, hper, hz),
         jnp.zeros((5, 128), f32)], axis=0)
    heads_t = heads.T[0:16]
    dtb, rate = heads_t[:, 0:1], heads_t[:, 1:2]
    gain_out = pick(ig_ref, per, None)
    spread = (lax.broadcasted_iota(jnp.int32, (48, VC), 1) // HEAD_DIM
              == lax.rem(lax.broadcasted_iota(jnp.int32, (48, VC), 0), 16)).astype(bf16)

    def thirds(m):
        top = m.astype(bf16).astype(f32)
        mid = (m - top).astype(bf16).astype(f32)
        return [top, mid, m - top - mid]

    def widen(parts):
        return jnp.dot(parts.astype(bf16), spread, preferred_element_type=f32)

    skip_wide = widen(jnp.concatenate(thirds(heads[:, 0:16]), axis=1))[2:3]
    ii = lax.broadcasted_iota(jnp.int32, (BLOCK, BLOCK), 0)
    jj = lax.broadcasted_iota(jnp.int32, (BLOCK, BLOCK), 1)
    causal = ii >= jj
    triu = (ii <= jj).astype(bf16)
    low_lane = lax.broadcasted_iota(jnp.int32, (BLOCK, 128), 1) < HEAD_DIM
    margin = CONV - 1

    def norm_in(k, h):
        v = sbuf[k, h].astype(f32)
        ms = jnp.mean(v * v, axis=-1, keepdims=True)
        nbuf[k, h] = (v * lax.rsqrt(ms + epsilon) * gain_in).astype(bf16)

    def unit(k, h, hook=None):
        nb = nbuf[k, h]
        if h == 0:
            cbuf[0:8, :] = jnp.zeros((8, CC), f32)
        else:
            cbuf[0:8, :] = tails[k]
        cbuf[8 : 8 + rows, :] = jnp.dot(nb, wbuf[...], preferred_element_type=f32).astype(bf16).astype(f32)
        if h == 0:
            tails[k] = cbuf[rows : rows + 8, :]
        acc = jnp.broadcast_to(tbias, (rows, CC))
        for t in range(CONV):
            acc = acc + taps[t : t + 1, :] * cbuf[8 - margin + t : 8 - margin + t + rows, :]
        vbuf[...] = (acc / (1.0 + jnp.exp(-acc))).astype(bf16)
        if hook is not None:
            hook()
        raw = lax.dot_general(w_steps, nb, (((1,), (1,)), ((), ())), preferred_element_type=f32) + dtb
        dt_t = jnp.maximum(raw, 0.0) + jnp.log1p(jnp.exp(-jnp.abs(raw)))
        sums = jnp.dot(jnp.concatenate(thirds(-dt_t * rate), axis=0).astype(bf16), triu, preferred_element_type=f32)
        cum_t = sums[0:16] + (sums[16:32] + sums[32:48])
        tail_t = jnp.exp(cum_t[:, BLOCK - 1 : BLOCK] - cum_t) * dt_t
        cols = jnp.concatenate([cum_t, *thirds(tail_t), *thirds(jnp.exp(cum_t)), jnp.zeros((16, BLOCK), f32)], axis=0).T
        cum = cols[:, 0:16]
        bm = vbuf[:, VC : VC + STATE]
        cm = vbuf[:, VC + STATE : CC]
        scores = lax.dot_general(cm, bm, (((1,), (1,)), ((), ())), preferred_element_type=f32)
        scores = jnp.where(causal, scores, 0.0)
        vals = vbuf[:, 0:VC].astype(f32)
        part = skip_wide * vals
        if h > 0:
            grow = widen(cols[:, 64:112])
            part = part + grow * jnp.dot(jnp.concatenate([cm, cm, cm], axis=1), state[k],
                                         preferred_element_type=f32)
        for p in range(VC // 128):
            mix = []
            for q in range(2):
                hd = 2 * p + q
                lag = cum[:, hd : hd + 1] - cum_t[hd : hd + 1, :]
                m = scores * jnp.exp(jnp.minimum(lag, 0.0)) * dt_t[hd : hd + 1, :]
                mix.append(m.astype(bf16))
            vp = vals[:, p * 128 : (p + 1) * 128]
            two = jnp.concatenate([jnp.where(low_lane, vp, 0.0), jnp.where(low_lane, 0.0, vp)],
                                  axis=0).astype(bf16)
            got = jnp.dot(jnp.concatenate(mix, axis=1), two, preferred_element_type=f32)
            ybuf[:, p * 128 : (p + 1) * 128] = got + part[:, p * 128 : (p + 1) * 128]
        y = ybuf[...]
        pbuf[k, h] = jnp.dot((y * gain_out).astype(bf16), wobuf[...], preferred_element_type=f32).astype(bf16)
        ones = jnp.ones((8, VC), bf16)
        stat = [lax.dot_general(ones, sq.astype(bf16), (((1,), (1,)), ((), ())), preferred_element_type=f32)
                for sq in thirds(y * y)]
        stbuf[k, h] = stat[0] + (stat[1] + stat[2])
        if h == 0:
            scaled = (vals * widen(cols[:, 16:64])).astype(bf16)
            whole = lax.dot_general(bm, scaled, (((0,), (0,)), ((), ())), preferred_element_type=f32)
            state[k] = jnp.concatenate(thirds(whole), axis=0).astype(bf16)

    def place(b, h):
        return {"dp": b, "seq": h}

    def here(h):
        return jnp.logical_and(own_core, h == c)

    def p_copies(h, whole=False):
        slot = lax.rem(z, S)
        where = place(2 * near + c, h)
        parts = 1 if whole else QP
        return (rcopy(stbuf.at[near, h], rstat.at[slot], t_send.at[near, h], t_recv.at[slot], where),
                *(rcopy(pbuf.at[near, h, band(q, parts)], rpart.at[slot, band(q, parts)], p_send.at[h],
                        p_recv.at[slot, q], where) for q in range(parts)))

    def x_copies(h, q):
        at, q = (band(0, 1), 0) if q is None else (band(q, QP), q)
        big = rcopy(pbuf.at[far, h, at], xpart.at[h, at], q_send.at[h], x_recv.at[h, q], {"dp": border})
        if q > 0:
            return (big,)
        return (rcopy(stbuf.at[far, h], xstat.at[h], t_send.at[far, h], y_recv.at[h], {"dp": border}), big)

    def b_copies(h, q, join):
        at, q = (band(0, 1), 0) if q is None else (band(q, QP), q)
        if join:
            where = {"dp": Z - 1 - z}
            big, small = (kpart.at[h, at], k_recv.at[h, q]), (kstat.at[h], kt_recv.at[h])
        else:
            where = place(2 * far + c, h)
            big, small = (rpart.at[S, at], p_recv.at[S, q]), (rstat.at[S], t_recv.at[S])
        big = rcopy(bpart.at[h, at], big[0], b_send.at[h], big[1], where)
        if q > 0:
            return (big,)
        return (rcopy(bstat.at[h], small[0], c_send.at[h], small[1], where), big)

    def j_copies(h, q):
        where = place(edge, h)
        at, q = (band(0, 1), 0) if q is None else (band(q, QP), q)
        big = rcopy(jpart.at[h, at], rpart.at[S, at], j_send.at[h], p_recv.at[S, q], where)
        if q > 0:
            return (big,)
        return (rcopy(jstat.at[h], rstat.at[S], jt_send.at[h], t_recv.at[S], where), big)

    def join_near(h, chunks=range(QP), on=True):
        @pl.when(jnp.logical_and(joiner, on))
        def _():
            for q in chunks:
                at = band(q, QP)
                for cp in b_copies(h, q, True):
                    cp.wait_recv()
                jpart[h, at] = (pbuf[near, h, at].astype(f32) + kpart[h, at].astype(f32)).astype(bf16)
                if q == 0:
                    jstat[h] = stbuf[near, h] + kstat[h]
                for cp in j_copies(h, q):
                    cp.start()

    def send_far(h):
        @pl.when(outer)
        def _():
            for q in range(QP):
                for cp in x_copies(h, q):
                    cp.start()

    def send_near(h, now):
        @pl.when(jnp.logical_and(now, here(h)))
        def _():
            rpart[lax.rem(z, S)] = pbuf[near, h]
            rstat[lax.rem(z, S)] = stbuf[near, h]

        @pl.when(jnp.logical_and(jnp.logical_and(now, jnp.logical_not(joiner)), jnp.logical_not(here(h))))
        def _():
            for cp in p_copies(h):
                cp.start()

    def sum_far(h, chunks=range(QP), on=True):
        @pl.when(jnp.logical_and(inner, on))
        def _():
            for q in chunks:
                at = band(q, QP)
                for cp in x_copies(h, q):
                    cp.wait_recv()
                bpart[h, at] = (pbuf[far, h, at].astype(f32) + xpart[h, at].astype(f32)).astype(bf16)
                if q == 0:
                    bstat[h] = stbuf[far, h] + xstat[h]
                for on, join in ((own_core, True), (jnp.logical_not(own_core), False)):
                    @pl.when(on)
                    def _():
                        for cp in b_copies(h, q, join):
                            cp.start()

    with scope("passf0i"):
        pass_at(far, 0, inner)
    with scope('passn1i'):
        pass_at(near, 1, joiner)
    for step in range(1, Z):
        for d in (z + step, z - step):
            @pl.when(jnp.logical_and(d >= 0, d < Z))
            def _():
                with scope(f"wrecv{step}"):
                    for cp in w_copies(z, d):
                        cp.wait_recv()
                for cp in f_copies(d, c):
                    cp.start()
    with scope("prewait"):
        send_x(jnp.logical_and(c == 1, inner), False)
        pass_at(far, 1, summer)
        pass_at(near, 1, summer)
        for q in range(QX):
            own_on(1, q, lambda cp: cp.start())
    with scope("fwait"):
        for cp in forwards():
            cp.wait_recv()
        wo_copy.wait_recv()
    w_steps = jnp.concatenate([dbuf[g][:, 0:KR].astype(f32) for g in range(2 * Z)], axis=1).astype(bf16)

    def r_copies(j, q):
        at = band(q, QP)
        big = rcopy(pbuf.at[0, 0, at], rpart.at[j, at], p_send.at[0], p_recv.at[j, q], sib)
        if q > 0:
            return (big,)
        return (rcopy(stbuf.at[0, 0], rstat.at[j], t_send.at[0, 0], t_recv.at[j], sib), big)

    def e_copy(q, parts=QP):
        at = band(q, parts)
        return rcopy(obuf.at[at], out_ref.at[at], e_send, e_recv, {"section": nxt})

    def finish():
        scale = None
        for q in range(QP):
            at = band(q, QP)
            with scope(f"rwait{q}"):
                for j in range(S + 1):
                    own = lax.rem(z, S) == j
                    take = jnp.logical_or(jnp.logical_and(own, jnp.logical_not(own_core)),
                                          jnp.logical_and(inner, jnp.logical_not(own))) if j < S else True
                    @pl.when(take)
                    def _():
                        for cp in r_copies(j, q):
                            cp.wait_recv()
            if q == 0:
                stat = rstat[S]
                for j in range(S):
                    stat = stat + jnp.where(jnp.logical_or(inner, lax.rem(z, S) == j), rstat[j], 0.0)
                scale = lax.rsqrt(stat * (1.0 / INNER) + epsilon).T[:, 0:1]
            total = rpart[S, at].astype(f32)
            for j in range(S):
                part = rpart[j, at].astype(f32)
                total = total + jnp.where(jnp.logical_or(inner, lax.rem(z, S) == j), part, 0.0)
            size = rows // QP
            obuf[at, :] = (x_ref[at].astype(f32) + total * scale[q * size : (q + 1) * size]).astype(bf16)
            e_copy(q).start()

    with scope("passn0"):
        pass_at(near, 0, outer)
    with scope("unit0"):
        norm_in(one, 0)
        unit(one, 0, lambda: pass_at(far, 1, joiner, (0,)))
    with scope("passf1i"):
        pass_at(far, 1, joiner, (1,))
    with scope("passf0"):
        pass_at(far, 0, outer)
    with scope("unit1"):
        norm_in(two, 0)
        unit(two, 0, lambda: pass_at(far, 1, joiner, (2,)))
    send_far(0)
    send_near(0, outer)
    with scope("passf1j"):
        pass_at(far, 1, joiner, (3,))
    with scope("sumf0"):
        sum_far(0)
    with scope("passf1"):
        pass_at(far, 1, outer)
    with scope("unit2"):
        norm_in(far, 1)
        unit(far, 1)
    send_far(1)
    with scope("sums1"):
        sum_far(1, on=summer)
    send_near(0, inner)
    with scope("passn1"):
        pass_at(near, 1, outer)
    with scope("unit3"):
        norm_in(near, 1)
        unit(near, 1)
    send_near(1, inner)
    send_near(1, outer)
    with scope("join0"):
        join_near(0)
    with scope("fin0"):
        @pl.when(c == 0)
        def _():
            finish()
    for q in range(QP):
        with scope("join1"):
            join_near(1, (q,), jnp.logical_not(upper))
        with scope("sumf1"):
            sum_far(1, (q,), joiner)
        with scope("join1u"):
            join_near(1, (q,), upper)
    with scope("fin1"):
        @pl.when(c == 1)
        def _():
            finish()
    with scope("sends"):
        for way, on in ways:
            on = on if way == 0 else jnp.logical_and(on, jnp.logical_or(outer, jnp.logical_xor(upper, way == 2)))
            @pl.when(on)
            def _():
                i_copy(None, way).wait_send()
        wo_copy.wait_send()
        for cp in forwards():
            cp.wait_send()
        others = pl.ds(0, Z - 1)
        rcopy(w2.at[others], w2.at[others], w_send, w_recv.at[0], sib).wait_send()
        rcopy(d2.at[others], d2.at[others], d_send, d_recv.at[0], sib).wait_send()
        for h in range(2):
            for k in range(S):
                relay(k, h, None, lambda cp: cp.wait_send())
            own_on(h, None, lambda cp: cp.wait_send())
            @pl.when(outer)
            def _():
                for cp in x_copies(h, None):
                    cp.wait_send()
            @pl.when(inner)
            def _():
                for cp in b_copies(h, None, True):
                    cp.wait_send()
            @pl.when(joiner)
            def _():
                for cp in j_copies(h, None):
                    cp.wait_send()
            @pl.when(jnp.logical_not(jnp.logical_or(joiner, here(h))))
            def _():
                for cp in p_copies(h, True):
                    cp.wait_send()
    with scope("last"):
        e_copy(0, 1).wait()


def fused(
    stream, norm_gain, w_xbc, w_dt, conv_weight, conv_bias, dt_bias, decay_rate, skip_weight,
    inner_gain, w_out,
):
    Z = lax.axis_size("dp")
    rows, D = stream.shape[2:]
    if rows != BLOCK:
        return shards(stream, norm_gain, w_xbc, w_dt, conv_weight, conv_bias, dt_bias, decay_rate,
                      skip_weight, inner_gain, w_out)
    KR = w_xbc.shape[1]
    VC = INNER // Z
    CC = VC + 2 * STATE
    S = Z // 2
    lanes = -(-KR // 128) * 128
    bf16, f32 = jnp.bfloat16, jnp.float32
    dma, V = pltpu.SemaphoreType.DMA, pltpu.VMEM
    far, held = pl.BlockSpec(memory_space=pltpu.HBM), pl.BlockSpec(memory_space=pltpu.VMEM)
    out = pl.pallas_call(
        functools.partial(section_kernel, Z),
        out_shape=jax.ShapeDtypeStruct((rows, D), bf16),
        in_specs=[far] * 11,
        out_specs=pl.BlockSpec(memory_space=pl.ANY),
        scratch_shapes=[
            V((rows, D), bf16), V(norm_gain.shape, f32), V(w_xbc.shape[1:], bf16),
            V((HEADS, KR), bf16), V(conv_weight.shape[1:], f32), V(conv_bias.shape, f32),
            V(dt_bias.shape, f32), V(dt_bias.shape, f32), V(dt_bias.shape, f32),
            V(inner_gain.shape, f32), V(w_out.shape[1:], bf16),
            V((Z, KR, CC), bf16), V((2 * Z * KR, CC), bf16),
            V((Z, 16, lanes), bf16), V((2 * Z, 16, lanes), bf16),
            V((VC, D), bf16),
            V((S, 2, rows, D), bf16), V((S, 2, rows, D), bf16),
            V((8 + rows, CC), f32), V((S, 8, CC), f32), V((rows, CC), bf16), V((rows, VC), f32),
            V((S, 3 * STATE, VC), bf16),
            V((S, 2, rows, D), bf16), V((S, 2, 8, rows), f32),
            V((2, rows, D), bf16), V((2, 8, rows), f32),
            V((2, rows, D), bf16), V((2, 8, rows), f32),
            V((2, rows, D), bf16), V((2, 8, rows), f32),
            V((2, rows, D), bf16), V((2, 8, rows), f32),
            V((S + 1, rows, D), bf16), V((S + 1, 8, rows), f32),
            V((rows, D), bf16),
            dma((11,)), dma, dma((Z,)), dma, dma((Z,)), dma, dma, dma, dma, dma, dma,
            dma((3,)), dma((S, 2)), dma((S, 2, QX)), dma, dma, dma((2,)), dma((S + 1, QP)),
            dma((S, 2)), dma((S + 1,)),
            dma((2,)), dma((2, QP)), dma((2,)), dma((2,)), dma((2,)), dma((2, QP)), dma((2,)),
            dma((2,)), dma((2,)),
        ],
        compiler_params=pltpu.CompilerParams(
            collective_id=0, has_side_effects=True, vmem_limit_bytes=50 * 1024 * 1024
        ),
    )(
        *(pltpu.with_memory_space_constraint(a, pltpu.HBM) for a in (
            stream[0, 0], norm_gain, w_xbc[0], jnp.swapaxes(w_dt, 1, 2)[0], conv_weight[0], conv_bias,
            dt_bias, decay_rate, skip_weight, inner_gain, w_out[0]))
    )
    return out[None, None]


def solution(mesh):
    placed = (
        P("section", "dp", "seq", None),
        P("section", None),
        P("section", ("seq", "dp"), None),
        P("section", ("seq", "dp"), None),
        P("section", None, None),
        P("section", None),
        P("section", None),
        P("section", None),
        P("section", None),
        P("section", None),
        P("section", ("seq", "dp"), None),
    )
    size = mesh.shape
    chips = size["dp"]
    whole_heads = HEADS % (2 * chips) == 0 and (INNER // chips) % 128 == 0
    body = fused if size["seq"] == 2 and chips == 4 and whole_heads and size["section"] > 1 else shards
    return jax.shard_map(
        body,
        mesh=mesh,
        in_specs=placed,
        out_specs=P("section", "dp", "seq", None),
        check_vma=False,
    )
```

```python
import functools

import jax
import jax.numpy as jnp
from jax import lax
from jax.experimental import pallas as pl
from jax.experimental.pallas import tpu as pltpu
from jax.sharding import PartitionSpec as P

HEADS = 40
HEAD_DIM = 64
STATE = 64
CONV = 4
BLOCK = 128
INNER = 2560


epsilon = 1e-05
QX = 2
QP = 8


def prefix(x, axis, combine, identity):
    devices, position = (lax.axis_size(axis), lax.axis_index(axis))
    everything = jax.tree.map(
        lambda part, kind: lax.all_gather(part.astype(kind), axis),
        x,
        jax.tree.map(lambda a: jnp.bfloat16 if a.dtype == jnp.float32 else a.dtype, x),
    )
    start = jax.tree.map(
        lambda part, zero: jnp.broadcast_to(jnp.asarray(zero, part.dtype), part.shape), x, identity
    )

    def hop(k, before):
        reached = k < position
        new = combine(
            before, jax.tree.map(lambda part, own: part[k].astype(own.dtype), everything, x)
        )
        return jax.tree.map(lambda a, b: jnp.where(reached, a, b), new, before)

    return lax.fori_loop(0, devices, hop, start)


def from_behind(x, axis, by):
    devices = lax.axis_size(axis)
    pairs = [(i, i + by) for i in range(devices) if 0 <= i + by < devices]
    return lax.ppermute(x, axis, pairs)


def passed_along(x, axis, by):
    devices = lax.axis_size(axis)
    return lax.ppermute(x, axis, [(i, (i + by) % devices) for i in range(devices)])


def rms_scale(values, scale_gain):
    mean_square = jnp.mean(values * values, axis=-1, keepdims=True)
    return values * lax.rsqrt(mean_square + epsilon) * scale_gain


def block_terms(values, b_rows, c_rows, dt_rows, head_rates):
    block_len = dt_rows.shape[0]
    cum_decay = jnp.cumsum(-dt_rows * head_rates[None, :], axis=0)
    scores = jnp.dot(c_rows, b_rows.T, preferred_element_type=jnp.float32)
    lag_decay = cum_decay.T[:, :, None] - cum_decay.T[:, None, :]
    causal = jnp.arange(block_len)[:, None] >= jnp.arange(block_len)[None, :]
    weights = jnp.where(causal[None], jnp.exp(jnp.minimum(lag_decay, 0.0)), 0.0)
    mixing = (scores[None] * weights * dt_rows.T[:, None, :]).astype(jnp.bfloat16)
    intra_out = jnp.einsum("hij,jhp->ihp", mixing, values, preferred_element_type=jnp.float32)
    tail_weight = jnp.exp(cum_decay[-1][None, :] - cum_decay) * dt_rows
    scaled = (values.astype(jnp.float32) * tail_weight[:, :, None]).astype(jnp.bfloat16)
    summary = jnp.einsum("jhp,jn->hpn", scaled, b_rows, preferred_element_type=jnp.float32)
    return (intra_out, summary, jnp.exp(cum_decay[-1]), jnp.exp(cum_decay))


def state_output(c_rows, growth, carried):
    readout = jnp.einsum(
        "in,hpn->ihp", c_rows.astype(jnp.float32), carried, precision=lax.Precision.HIGHEST
    )
    return growth[:, :, None] * readout


def combine_states(earlier, latest):
    decay_a, state_a = earlier
    decay_b, state_b = latest
    return (decay_a * decay_b, decay_b[:, None] * state_a + state_b)


def chain_states(summary):
    identity = (jnp.ones_like(summary[0]), jnp.zeros_like(summary[1]))
    return prefix(summary, "seq", combine_states, identity)


def project_rows(normed_rows, xbc_part, dt_part):
    return (
        jnp.dot(
            normed_rows,
            lax.all_gather(xbc_part, ("seq", "dp"), axis=0, tiled=True),
            preferred_element_type=jnp.float32,
        ),
        jnp.dot(
            normed_rows,
            lax.all_gather(dt_part, ("seq", "dp"), axis=0, tiled=True),
            preferred_element_type=jnp.float32,
        ),
    )


def shards(
    stream,
    norm_gain,
    w_xbc,
    w_dt,
    conv_weight,
    conv_bias,
    dt_bias,
    decay_rate,
    skip_weight,
    inner_gain,
    w_out,
):
    rows_in = stream[0, 0]
    length_dev = rows_in.shape[0]
    margin = CONV - 1
    row_gain = norm_gain[0]
    normed = rms_scale(rows_in.astype(jnp.float32), row_gain).astype(jnp.bfloat16)
    projected, dt_raw = project_rows(normed, w_xbc[0], w_dt[0])
    xbc_raw = projected.astype(jnp.bfloat16)
    prev_proj = from_behind(xbc_raw[length_dev - margin :], "seq", 1)
    padded = jnp.concatenate([prev_proj, xbc_raw], axis=0)
    conv_sum = jnp.broadcast_to(conv_bias[0][None, :], (length_dev, padded.shape[1]))
    for tap_index in range(CONV):
        conv_sum = conv_sum + conv_weight[0, tap_index][None, :] * padded[
            tap_index : tap_index + length_dev
        ].astype(jnp.float32)
    mixed_rows = jax.nn.silu(conv_sum).astype(jnp.bfloat16)
    blocks = length_dev // BLOCK
    values = mixed_rows[:, :INNER].reshape(blocks, BLOCK, HEADS, HEAD_DIM)
    b_rows = mixed_rows[:, INNER : INNER + STATE].reshape(blocks, BLOCK, STATE)
    c_rows = mixed_rows[:, INNER + STATE :].reshape(blocks, BLOCK, STATE)
    dt_rows = jax.nn.softplus(dt_raw + dt_bias[0][None, :]).reshape(blocks, BLOCK, HEADS)
    intra_out, summary, totals, growth = jax.vmap(block_terms, in_axes=(0, 0, 0, 0, None))(
        values, b_rows, c_rows, dt_rows, decay_rate[0]
    )

    def local_step(running, inputs):
        carried, decay_before = running
        block_total, block_summary = inputs
        return (
            (block_total[:, None, None] * carried + block_summary, decay_before * block_total),
            (carried, decay_before),
        )

    start_state = (
        jnp.zeros((HEADS, HEAD_DIM, STATE), jnp.float32),
        jnp.ones((HEADS,), jnp.float32),
    )
    (local_state, local_decay), (enter_local, decay_before) = lax.scan(
        local_step, start_state, (totals, summary)
    )
    state_terms = jax.vmap(state_output)
    early_terms = state_terms(c_rows, growth, enter_local)
    incoming_decay, incoming_flat = chain_states(
        (local_decay, local_state.reshape(HEADS, HEAD_DIM * STATE))
    )
    arriving = incoming_flat.reshape(HEADS, HEAD_DIM, STATE)
    late_terms = state_terms(c_rows, growth, decay_before[:, :, None, None] * arriving[None])
    state_part = early_terms + late_terms
    mixed_out = (
        intra_out + state_part + skip_weight[0][None, None, :, None] * values.astype(jnp.float32)
    )
    normed_out = rms_scale(mixed_out.reshape(length_dev, INNER), inner_gain[0]).astype(jnp.bfloat16)
    branch_out = jnp.dot(
        normed_out,
        lax.all_gather(w_out[0], ("seq", "dp"), axis=0, tiled=True),
        preferred_element_type=jnp.float32,
    )
    next_rows = (rows_in.astype(jnp.float32) + branch_out).astype(jnp.bfloat16)
    shifted = passed_along(next_rows, "section", 1)
    return shifted[None, None]

def section_kernel(
    Z, x_hbm, ng_hbm, w_hbm, wd_hbm, cw_hbm, cb_hbm, db_hbm, dr_hbm, sk_hbm, ig_hbm, wo_hbm,
    out_ref,
    x_ref, ng_ref, w_ref, wd_ref, cw_ref, cb_ref, db_ref, dr_ref, sk_ref, ig_ref, wo_ref, w2,
    wbuf, d2, dbuf, wobuf, sbuf, nbuf, cbuf, tails, vbuf, ybuf, state,
    pbuf, stbuf, xpart, xstat, bpart, bstat, kpart, kstat, jpart, jstat, rpart, rstat, obuf,
    l_sem, w_send, w_recv, d_send, d_recv, f_send, f_recv, g_send, g_recv, o_send, o_recv,
    i_send, s_send, s_recv, e_send, e_recv, p_send, p_recv, t_send, t_recv,
    q_send, x_recv, y_recv, b_send, c_send, k_recv, kt_recv, j_send, jt_send,
):
    z = lax.axis_index("dp")
    c = lax.axis_index("seq")
    sec = lax.axis_index("section")
    NS = lax.axis_size("section")
    nxt = lax.rem(sec + 1, NS)
    prv = lax.rem(sec + NS - 1, NS)
    S = Z // 2
    rows, D = x_ref.shape
    KR = w_ref.shape[0]
    per = INNER // (2 * Z)
    hper = HEADS // (2 * Z)
    VC = 2 * per
    NB = 2 * STATE
    CC = VC + NB
    f32, bf16 = jnp.float32, jnp.bfloat16
    core = lax.rem(z, 2)
    own_core = core == c
    myslot = z // 2
    sib = {"seq": 1 - c}
    upper = z >= S
    border = jnp.where(upper, S, S - 1)
    edge = jnp.where(upper, Z - 1, 0)
    near = jnp.where(upper, S - 1, 0)
    far = 1 - near
    scope = jax.named_scope

    def rcopy(src, dst, ss, rs, where):
        return pltpu.make_async_remote_copy(
            src_ref=src, dst_ref=dst, send_sem=ss, recv_sem=rs, device_id=where,
            device_id_type=pl.DeviceIdType.MESH,
        )

    def band(q, parts):
        return pl.ds(q * (rows // parts), rows // parts)

    loads = [
        pltpu.make_async_copy(src, dst, l_sem.at[i])
        for i, (src, dst) in enumerate((
            (x_hbm, x_ref), (w_hbm, w_ref), (wd_hbm, wd_ref), (wo_hbm, wo_ref), (ng_hbm, ng_ref),
            (cw_hbm, cw_ref), (cb_hbm, cb_ref), (db_hbm, db_ref), (dr_hbm, dr_ref), (sk_hbm, sk_ref),
            (ig_hbm, ig_ref)))
    ]
    for load in loads:
        load.start()
    barrier = pltpu.get_barrier_semaphore()
    for d in range(Z):
        for e in range(2):
            @pl.when(jnp.logical_not(jnp.logical_and(d == z, e == c)))
            def _():
                pl.semaphore_signal(barrier, inc=1, device_id={"dp": d, "seq": e},
                                    device_id_type=pl.DeviceIdType.MESH)
    for s in (nxt, prv):
        pl.semaphore_signal(barrier, inc=1, device_id={"section": s},
                            device_id_type=pl.DeviceIdType.MESH)

    def row0(core, chip):
        return pl.multiple_of((core * Z + chip) * KR, KR)

    lanes = d2.shape[2]
    loads[2].wait()
    for d in range(Z):
        two = jnp.concatenate(
            [wd_ref[d * hper : (d + 1) * hper, :].astype(f32),
             wd_ref[(Z + d) * hper : (Z + d + 1) * hper, :].astype(f32),
             jnp.zeros((16 - 2 * hper, KR), f32)], axis=0)
        d2[d] = jnp.concatenate([two, jnp.zeros((16, lanes - KR), f32)], axis=1).astype(bf16)
    dbuf[c * Z + z] = d2[z]
    loads[0].wait()
    loads[1].wait()
    for d in range(Z):
        w2[d, :, 0:per] = w_ref[:, d * per : (d + 1) * per]
        w2[d, :, per:VC] = w_ref[:, Z * per + d * per : Z * per + (d + 1) * per]
        w2[d, :, VC:CC] = w_ref[:, INNER : INNER + NB]

    with scope("barrier"):
        pl.semaphore_wait(barrier, 2 * Z - 1 + 2)

    def i_copy(q, way):
        where = sib if way == 0 else {"dp": z + (1 if way == 1 else -1), "seq": core}
        at = band(0, 1) if q is None else band(q, QX)
        q = q or 0
        return rcopy(x_ref.at[at], sbuf.at[myslot, c, at], i_send.at[way], s_recv.at[myslot, c, q], where)

    inner, outer = z == border, z != border
    ways = ((0, jnp.logical_not(own_core)), (1, z + 1 < Z), (2, z > 0))
    summer = jnp.logical_and(inner, own_core)
    joiner = jnp.logical_and(inner, jnp.logical_not(own_core))

    def send_x(on, inward):
        for way, there in ways[1:]:
            towards = jnp.logical_xor(upper, way == 1)
            if inward:
                there = jnp.logical_and(there, outer)
            @pl.when(jnp.logical_and(jnp.logical_and(on, there), towards if inward else jnp.logical_not(towards)))
            def _():
                for q in range(QX):
                    i_copy(q, way).start()

    def s_copy(k, h, q, up):
        at = band(0, 1) if q is None else band(q, QX)
        q = q or 0
        return rcopy(sbuf.at[k, h, at], sbuf.at[k, h, at], s_send.at[k, h], s_recv.at[k, h, q],
                     {"dp": z + (1 if up else -1)})

    def relay(k, h, q, fn):
        b = 2 * k + c
        @pl.when(jnp.logical_and(z > b, z + 1 < Z))
        def _():
            fn(s_copy(k, h, q, True))
        @pl.when(jnp.logical_and(z < b, z > 0))
        def _():
            fn(s_copy(k, h, q, False))

    def own_on(h, q, fn):
        at = band(0, 1) if q is None else band(q, QX)
        @pl.when(summer)
        def _():
            fn(rcopy(sbuf.at[near, h, at], sbuf.at[near, h, at], s_send.at[near, h],
                     s_recv.at[near, h, q or 0], {"dp": jnp.where(upper, z - 1, z + 1)}))

    def pass_on(k, h, chunks=range(QX)):
        for q in chunks:
            @pl.when(jnp.logical_not(jnp.logical_and(own_core, jnp.logical_and(k == myslot, h == c))))
            def _():
                s_copy(k, h, q, True).wait_recv()
            relay(k, h, q, lambda cp: cp.start())


    def pass_at(k, h, on, chunks=range(QX)):
        @pl.when(on)
        def _():
            pass_on(k, h, chunks)

    one, two = jnp.where(inner, far, near), jnp.where(inner, near, far)

    def w_copies(d, frm):
        at = pl.ds(row0(c, frm), KR)
        g = c * Z + frm
        return (rcopy(w2.at[d], wbuf.at[at], w_send, w_recv.at[frm], {"dp": d}),
                rcopy(d2.at[d], dbuf.at[g], d_send, d_recv.at[frm], {"dp": d}))

    def f_copies(d, core):
        at = pl.ds(row0(core, d), KR)
        g = core * Z + d
        return (rcopy(wbuf.at[at], wbuf.at[at], f_send, f_recv, sib),
                rcopy(dbuf.at[g], dbuf.at[g], g_send, g_recv, sib))

    def forwards():
        half = pl.ds(0, Z * KR)
        return (rcopy(wbuf.at[half], wbuf.at[half], f_send, f_recv, sib),
                rcopy(dbuf.at[pl.ds(0, Z)], dbuf.at[pl.ds(0, Z)], g_send, g_recv, sib))

    def send_w(d, on):
        @pl.when(on)
        def _():
            for cp in w_copies(d, z):
                cp.start()

    @pl.when(own_core)
    def _():
        sbuf[myslot, c] = x_ref[...]

    with scope("early"):
        @pl.when(ways[0][1])
        def _():
            for q in range(QX):
                i_copy(q, 0).start()
        send_x(c == 0, True)
        send_x(c == 0, False)
        @pl.when(c == 0)
        def _():
            for q in range(QX):
                own_on(0, q, lambda cp: cp.start())
        send_w(jnp.where(upper, 0, Z - 1), inner)
        send_w(edge, inner)
        for step in (3, 1, 2):
            send_w(jnp.where(upper, z - step, z + step), outer)
        own_fwd = (
            rcopy(w2.at[z], wbuf.at[pl.ds(row0(c, z), KR)], f_send, f_recv, sib),
            rcopy(d2.at[z], dbuf.at[c * Z + z], g_send, g_recv, sib),
        )
        for cp in own_fwd:
            cp.start()
        wbuf[pl.ds(row0(c, z), KR), :] = w2[z]
        pass_at(near, 0, inner)
        @pl.when(c == 1)
        def _():
            for q in range(QX):
                own_on(0, q, lambda cp: cp.start())
        send_w(jnp.where(upper, S - 1, S), inner)
        send_x(jnp.logical_and(c == 1, outer), True)

    loads[3].wait()
    at_wo = pl.ds(pl.multiple_of(c * per, per), per)
    wo_copy = rcopy(wo_ref, wobuf.at[at_wo], o_send, o_recv, sib)
    wo_copy.start()
    wobuf[at_wo, :] = wo_ref[...]
    for load in loads[4:]:
        load.wait()

    def pick(ref, width, tail):
        wide = Z * width
        got = None
        for d in range(Z):
            part = jnp.concatenate(
                [ref[:, d * width : (d + 1) * width],
                 ref[:, wide + d * width : wide + (d + 1) * width]], axis=1)
            part = jnp.where(z == d, part, 0.0)
            got = part if got is None else got + part
        return jnp.concatenate([got, tail], axis=1) if tail is not None else got

    gain_in = ng_ref[...]
    taps = pick(cw_ref, per, cw_ref[:, INNER : INNER + NB])
    tbias = pick(cb_ref, per, cb_ref[:, INNER : INNER + NB])
    hz = jnp.zeros((1, 128 - 2 * hper), f32)
    heads = jnp.concatenate(
        [pick(db_ref, hper, hz), pick(dr_ref, hper, hz), pick(sk_ref, hper, hz),
         jnp.zeros((5, 128), f32)], axis=0)
    heads_t = heads.T[0:16]
    dtb, rate = heads_t[:, 0:1], heads_t[:, 1:2]
    gain_out = pick(ig_ref, per, None)
    spread = (lax.broadcasted_iota(jnp.int32, (48, VC), 1) // HEAD_DIM
              == lax.rem(lax.broadcasted_iota(jnp.int32, (48, VC), 0), 16)).astype(bf16)

    def thirds(m):
        top = m.astype(bf16).astype(f32)
        mid = (m - top).astype(bf16).astype(f32)
        return [top, mid, m - top - mid]

    def widen(parts):
        return jnp.dot(parts.astype(bf16), spread, preferred_element_type=f32)

    skip_wide = widen(jnp.concatenate(thirds(heads[:, 0:16]), axis=1))[2:3]
    ii = lax.broadcasted_iota(jnp.int32, (BLOCK, BLOCK), 0)
    jj = lax.broadcasted_iota(jnp.int32, (BLOCK, BLOCK), 1)
    causal = ii >= jj
    triu = (ii <= jj).astype(bf16)
    low_lane = lax.broadcasted_iota(jnp.int32, (BLOCK, 128), 1) < HEAD_DIM
    margin = CONV - 1

    def norm_in(k, h):
        v = sbuf[k, h].astype(f32)
        ms = jnp.mean(v * v, axis=-1, keepdims=True)
        nbuf[k, h] = (v * lax.rsqrt(ms + epsilon) * gain_in).astype(bf16)

    def unit(k, h, hook=None):
        nb = nbuf[k, h]
        if h == 0:
            cbuf[0:8, :] = jnp.zeros((8, CC), f32)
        else:
            cbuf[0:8, :] = tails[k]
        cbuf[8 : 8 + rows, :] = jnp.dot(nb, wbuf[...], preferred_element_type=f32).astype(bf16).astype(f32)
        if h == 0:
            tails[k] = cbuf[rows : rows + 8, :]
        acc = jnp.broadcast_to(tbias, (rows, CC))
        for t in range(CONV):
            acc = acc + taps[t : t + 1, :] * cbuf[8 - margin + t : 8 - margin + t + rows, :]
        vbuf[...] = (acc / (1.0 + jnp.exp(-acc))).astype(bf16)
        if hook is not None:
            hook()
        raw = lax.dot_general(w_steps, nb, (((1,), (1,)), ((), ())), preferred_element_type=f32) + dtb
        dt_t = jnp.maximum(raw, 0.0) + jnp.log1p(jnp.exp(-jnp.abs(raw)))
        sums = jnp.dot(jnp.concatenate(thirds(-dt_t * rate), axis=0).astype(bf16), triu, preferred_element_type=f32)
        cum_t = sums[0:16] + (sums[16:32] + sums[32:48])
        tail_t = jnp.exp(cum_t[:, BLOCK - 1 : BLOCK] - cum_t) * dt_t
        cols = jnp.concatenate([cum_t, *thirds(tail_t), *thirds(jnp.exp(cum_t)), jnp.zeros((16, BLOCK), f32)], axis=0).T
        cum = cols[:, 0:16]
        bm = vbuf[:, VC : VC + STATE]
        cm = vbuf[:, VC + STATE : CC]
        scores = lax.dot_general(cm, bm, (((1,), (1,)), ((), ())), preferred_element_type=f32)
        scores = jnp.where(causal, scores, 0.0)
        vals = vbuf[:, 0:VC].astype(f32)
        part = skip_wide * vals
        if h > 0:
            grow = widen(cols[:, 64:112])
            part = part + grow * jnp.dot(jnp.concatenate([cm, cm, cm], axis=1), state[k],
                                         preferred_element_type=f32)
        for p in range(VC // 128):
            mix = []
            for q in range(2):
                hd = 2 * p + q
                lag = cum[:, hd : hd + 1] - cum_t[hd : hd + 1, :]
                m = scores * jnp.exp(jnp.minimum(lag, 0.0)) * dt_t[hd : hd + 1, :]
                mix.append(m.astype(bf16))
            vp = vals[:, p * 128 : (p + 1) * 128]
            two = jnp.concatenate([jnp.where(low_lane, vp, 0.0), jnp.where(low_lane, 0.0, vp)],
                                  axis=0).astype(bf16)
            got = jnp.dot(jnp.concatenate(mix, axis=1), two, preferred_element_type=f32)
            ybuf[:, p * 128 : (p + 1) * 128] = got + part[:, p * 128 : (p + 1) * 128]
        y = ybuf[...]
        pbuf[k, h] = jnp.dot((y * gain_out).astype(bf16), wobuf[...], preferred_element_type=f32).astype(bf16)
        ones = jnp.ones((8, VC), bf16)
        stat = [lax.dot_general(ones, sq.astype(bf16), (((1,), (1,)), ((), ())), preferred_element_type=f32)
                for sq in thirds(y * y)]
        stbuf[k, h] = stat[0] + (stat[1] + stat[2])
        if h == 0:
            scaled = (vals * widen(cols[:, 16:64])).astype(bf16)
            whole = lax.dot_general(bm, scaled, (((0,), (0,)), ((), ())), preferred_element_type=f32)
            state[k] = jnp.concatenate(thirds(whole), axis=0).astype(bf16)

    def place(b, h):
        return {"dp": b, "seq": h}

    def here(h):
        return jnp.logical_and(own_core, h == c)

    def p_copies(h, whole=False):
        slot = lax.rem(z, S)
        where = place(2 * near + c, h)
        parts = 1 if whole else QP
        return (rcopy(stbuf.at[near, h], rstat.at[slot], t_send.at[near, h], t_recv.at[slot], where),
                *(rcopy(pbuf.at[near, h, band(q, parts)], rpart.at[slot, band(q, parts)], p_send.at[h],
                        p_recv.at[slot, q], where) for q in range(parts)))

    def x_copies(h, q):
        at, q = (band(0, 1), 0) if q is None else (band(q, QP), q)
        big = rcopy(pbuf.at[far, h, at], xpart.at[h, at], q_send.at[h], x_recv.at[h, q], {"dp": border})
        if q > 0:
            return (big,)
        return (rcopy(stbuf.at[far, h], xstat.at[h], t_send.at[far, h], y_recv.at[h], {"dp": border}), big)

    def b_copies(h, q, join):
        at, q = (band(0, 1), 0) if q is None else (band(q, QP), q)
        if join:
            where = {"dp": Z - 1 - z}
            big, small = (kpart.at[h, at], k_recv.at[h, q]), (kstat.at[h], kt_recv.at[h])
        else:
            where = place(2 * far + c, h)
            big, small = (rpart.at[S, at], p_recv.at[S, q]), (rstat.at[S], t_recv.at[S])
        big = rcopy(bpart.at[h, at], big[0], b_send.at[h], big[1], where)
        if q > 0:
            return (big,)
        return (rcopy(bstat.at[h], small[0], c_send.at[h], small[1], where), big)

    def j_copies(h, q):
        where = place(edge, h)
        at, q = (band(0, 1), 0) if q is None else (band(q, QP), q)
        big = rcopy(jpart.at[h, at], rpart.at[S, at], j_send.at[h], p_recv.at[S, q], where)
        if q > 0:
            return (big,)
        return (rcopy(jstat.at[h], rstat.at[S], jt_send.at[h], t_recv.at[S], where), big)

    def join_near(h, chunks=range(QP), on=True):
        @pl.when(jnp.logical_and(joiner, on))
        def _():
            for q in chunks:
                at = band(q, QP)
                for cp in b_copies(h, q, True):
                    cp.wait_recv()
                jpart[h, at] = (pbuf[near, h, at].astype(f32) + kpart[h, at].astype(f32)).astype(bf16)
                if q == 0:
                    jstat[h] = stbuf[near, h] + kstat[h]
                for cp in j_copies(h, q):
                    cp.start()

    def send_far(h):
        @pl.when(outer)
        def _():
            for q in range(QP):
                for cp in x_copies(h, q):
                    cp.start()

    def send_near(h, now):
        @pl.when(jnp.logical_and(now, here(h)))
        def _():
            rpart[lax.rem(z, S)] = pbuf[near, h]
            rstat[lax.rem(z, S)] = stbuf[near, h]

        @pl.when(jnp.logical_and(jnp.logical_and(now, jnp.logical_not(joiner)), jnp.logical_not(here(h))))
        def _():
            for cp in p_copies(h):
                cp.start()

    def sum_far(h, chunks=range(QP), on=True):
        @pl.when(jnp.logical_and(inner, on))
        def _():
            for q in chunks:
                at = band(q, QP)
                for cp in x_copies(h, q):
                    cp.wait_recv()
                bpart[h, at] = (pbuf[far, h, at].astype(f32) + xpart[h, at].astype(f32)).astype(bf16)
                if q == 0:
                    bstat[h] = stbuf[far, h] + xstat[h]
                for on, join in ((own_core, True), (jnp.logical_not(own_core), False)):
                    @pl.when(on)
                    def _():
                        for cp in b_copies(h, q, join):
                            cp.start()

    with scope("passf0i"):
        pass_at(far, 0, inner)
    with scope('passn1i'):
        pass_at(near, 1, joiner)
    for step in range(1, Z):
        for d in (z + step, z - step):
            @pl.when(jnp.logical_and(d >= 0, d < Z))
            def _():
                with scope(f"wrecv{step}"):
                    for cp in w_copies(z, d):
                        cp.wait_recv()
                for cp in f_copies(d, c):
                    cp.start()
    with scope("prewait"):
        send_x(jnp.logical_and(c == 1, inner), False)
        pass_at(far, 1, summer)
        pass_at(near, 1, summer)
        for q in range(QX):
            own_on(1, q, lambda cp: cp.start())
    with scope("fwait"):
        for cp in forwards():
            cp.wait_recv()
        wo_copy.wait_recv()
    w_steps = jnp.concatenate([dbuf[g][:, 0:KR].astype(f32) for g in range(2 * Z)], axis=1).astype(bf16)

    def r_copies(j, q):
        at = band(q, QP)
        big = rcopy(pbuf.at[0, 0, at], rpart.at[j, at], p_send.at[0], p_recv.at[j, q], sib)
        if q > 0:
            return (big,)
        return (rcopy(stbuf.at[0, 0], rstat.at[j], t_send.at[0, 0], t_recv.at[j], sib), big)

    def e_copy(q, parts=QP):
        at = band(q, parts)
        return rcopy(obuf.at[at], out_ref.at[at], e_send, e_recv, {"section": nxt})

    def finish():
        scale = None
        for q in range(QP):
            at = band(q, QP)
            with scope(f"rwait{q}"):
                for j in range(S + 1):
                    own = lax.rem(z, S) == j
                    take = jnp.logical_or(jnp.logical_and(own, jnp.logical_not(own_core)),
                                          jnp.logical_and(inner, jnp.logical_not(own))) if j < S else True
                    @pl.when(take)
                    def _():
                        for cp in r_copies(j, q):
                            cp.wait_recv()
            if q == 0:
                stat = rstat[S]
                for j in range(S):
                    stat = stat + jnp.where(jnp.logical_or(inner, lax.rem(z, S) == j), rstat[j], 0.0)
                scale = lax.rsqrt(stat * (1.0 / INNER) + epsilon).T[:, 0:1]
            total = rpart[S, at].astype(f32)
            for j in range(S):
                part = rpart[j, at].astype(f32)
                total = total + jnp.where(jnp.logical_or(inner, lax.rem(z, S) == j), part, 0.0)
            size = rows // QP
            obuf[at, :] = (x_ref[at].astype(f32) + total * scale[q * size : (q + 1) * size]).astype(bf16)
            e_copy(q).start()

    with scope("passn0"):
        pass_at(near, 0, outer)
    with scope("unit0"):
        norm_in(one, 0)
        unit(one, 0, lambda: pass_at(far, 1, joiner, (0,)))
    with scope("passf1i"):
        None
    with scope("passf0"):
        pass_at(far, 0, outer)
    with scope("unit1"):
        norm_in(two, 0)
        unit(two, 0, lambda: pass_at(far, 1, joiner, (1,)))
    send_far(0)
    send_near(0, outer)
    with scope("passf1j"):
        None
    with scope("sumf0"):
        sum_far(0)
    with scope("passf1"):
        pass_at(far, 1, outer)
    with scope("unit2"):
        norm_in(far, 1)
        unit(far, 1)
    send_far(1)
    with scope("sums1"):
        sum_far(1, on=summer)
    send_near(0, inner)
    with scope("passn1"):
        pass_at(near, 1, outer)
    with scope("unit3"):
        norm_in(near, 1)
        unit(near, 1)
    send_near(1, inner)
    send_near(1, outer)
    with scope("join0"):
        join_near(0)
    with scope("fin0"):
        @pl.when(c == 0)
        def _():
            finish()
    for q in range(QP):
        with scope("join1"):
            join_near(1, (q,), jnp.logical_not(upper))
        with scope("sumf1"):
            sum_far(1, (q,), joiner)
        with scope("join1u"):
            join_near(1, (q,), upper)
    with scope("fin1"):
        @pl.when(c == 1)
        def _():
            finish()
    with scope("sends"):
        for way, on in ways:
            on = on if way == 0 else jnp.logical_and(on, jnp.logical_or(outer, jnp.logical_xor(upper, way == 2)))
            @pl.when(on)
            def _():
                i_copy(None, way).wait_send()
        wo_copy.wait_send()
        for cp in forwards():
            cp.wait_send()
        others = pl.ds(0, Z - 1)
        rcopy(w2.at[others], w2.at[others], w_send, w_recv.at[0], sib).wait_send()
        rcopy(d2.at[others], d2.at[others], d_send, d_recv.at[0], sib).wait_send()
        for h in range(2):
            for k in range(S):
                relay(k, h, None, lambda cp: cp.wait_send())
            own_on(h, None, lambda cp: cp.wait_send())
            @pl.when(outer)
            def _():
                for cp in x_copies(h, None):
                    cp.wait_send()
            @pl.when(inner)
            def _():
                for cp in b_copies(h, None, True):
                    cp.wait_send()
            @pl.when(joiner)
            def _():
                for cp in j_copies(h, None):
                    cp.wait_send()
            @pl.when(jnp.logical_not(jnp.logical_or(joiner, here(h))))
            def _():
                for cp in p_copies(h, True):
                    cp.wait_send()
    with scope("last"):
        e_copy(0, 1).wait()


def fused(
    stream, norm_gain, w_xbc, w_dt, conv_weight, conv_bias, dt_bias, decay_rate, skip_weight,
    inner_gain, w_out,
):
    Z = lax.axis_size("dp")
    rows, D = stream.shape[2:]
    if rows != BLOCK:
        return shards(stream, norm_gain, w_xbc, w_dt, conv_weight, conv_bias, dt_bias, decay_rate,
                      skip_weight, inner_gain, w_out)
    KR = w_xbc.shape[1]
    VC = INNER // Z
    CC = VC + 2 * STATE
    S = Z // 2
    lanes = -(-KR // 128) * 128
    bf16, f32 = jnp.bfloat16, jnp.float32
    dma, V = pltpu.SemaphoreType.DMA, pltpu.VMEM
    far, held = pl.BlockSpec(memory_space=pltpu.HBM), pl.BlockSpec(memory_space=pltpu.VMEM)
    out = pl.pallas_call(
        functools.partial(section_kernel, Z),
        out_shape=jax.ShapeDtypeStruct((rows, D), bf16),
        in_specs=[far] * 11,
        out_specs=pl.BlockSpec(memory_space=pl.ANY),
        scratch_shapes=[
            V((rows, D), bf16), V(norm_gain.shape, f32), V(w_xbc.shape[1:], bf16),
            V((HEADS, KR), bf16), V(conv_weight.shape[1:], f32), V(conv_bias.shape, f32),
            V(dt_bias.shape, f32), V(dt_bias.shape, f32), V(dt_bias.shape, f32),
            V(inner_gain.shape, f32), V(w_out.shape[1:], bf16),
            V((Z, KR, CC), bf16), V((2 * Z * KR, CC), bf16),
            V((Z, 16, lanes), bf16), V((2 * Z, 16, lanes), bf16),
            V((VC, D), bf16),
            V((S, 2, rows, D), bf16), V((S, 2, rows, D), bf16),
            V((8 + rows, CC), f32), V((S, 8, CC), f32), V((rows, CC), bf16), V((rows, VC), f32),
            V((S, 3 * STATE, VC), bf16),
            V((S, 2, rows, D), bf16), V((S, 2, 8, rows), f32),
            V((2, rows, D), bf16), V((2, 8, rows), f32),
            V((2, rows, D), bf16), V((2, 8, rows), f32),
            V((2, rows, D), bf16), V((2, 8, rows), f32),
            V((2, rows, D), bf16), V((2, 8, rows), f32),
            V((S + 1, rows, D), bf16), V((S + 1, 8, rows), f32),
            V((rows, D), bf16),
            dma((11,)), dma, dma((Z,)), dma, dma((Z,)), dma, dma, dma, dma, dma, dma,
            dma((3,)), dma((S, 2)), dma((S, 2, QX)), dma, dma, dma((2,)), dma((S + 1, QP)),
            dma((S, 2)), dma((S + 1,)),
            dma((2,)), dma((2, QP)), dma((2,)), dma((2,)), dma((2,)), dma((2, QP)), dma((2,)),
            dma((2,)), dma((2,)),
        ],
        compiler_params=pltpu.CompilerParams(
            collective_id=0, has_side_effects=True, vmem_limit_bytes=50 * 1024 * 1024
        ),
    )(
        *(pltpu.with_memory_space_constraint(a, pltpu.HBM) for a in (
            stream[0, 0], norm_gain, w_xbc[0], jnp.swapaxes(w_dt, 1, 2)[0], conv_weight[0], conv_bias,
            dt_bias, decay_rate, skip_weight, inner_gain, w_out[0]))
    )
    return out[None, None]


def solution(mesh):
    placed = (
        P("section", "dp", "seq", None),
        P("section", None),
        P("section", ("seq", "dp"), None),
        P("section", ("seq", "dp"), None),
        P("section", None, None),
        P("section", None),
        P("section", None),
        P("section", None),
        P("section", None),
        P("section", None),
        P("section", ("seq", "dp"), None),
    )
    size = mesh.shape
    chips = size["dp"]
    whole_heads = HEADS % (2 * chips) == 0 and (INNER // chips) % 128 == 0
    body = fused if size["seq"] == 2 and chips == 4 and whole_heads and size["section"] > 1 else shards
    return jax.shard_map(
        body,
        mesh=mesh,
        in_specs=placed,
        out_specs=P("section", "dp", "seq", None),
        check_vma=False,
    )
```
